32 devices in a mesh: row: 4 (over x, core), col: 4 (over z), depth: 2 (over y).
Axes of the slice: x: 2, y: 2, z: 4, core: 2. Of those that a mesh axis runs over, the one named last changes fastest.
Arguments:
- acts: bfloat16 [256, 32768], P('depth', 'row'), may hold values from -6 to 6
- act_mask: int32 [256, 256], P('depth', 'row'), may hold values 0 or 1
- w1: bfloat16 [256, 32, 128, 128], P(('row', 'depth'), 'col'), may hold values from -0.09375 to 0.09375
- cols1: int32 [256, 32], P('row', 'col'), may hold values from 0 to 255, as said below
- bias1: float32 [32768], P('col'), may hold values from -3 to 3
- mask2: int32 [256, 256], P('depth', 'col'), may hold values 0 or 1
- w2: bfloat16 [256, 32, 128, 128], P(('col', 'depth'), 'row'), may hold values from -0.1875 to 0.1875
- cols2: int32 [256, 32], P('col', 'row'), may hold values from 0 to 255, as said below
- bias2: float32 [32768], P(('row', 'col')), may hold values from -3 to 3
Outputs:
- result: bfloat16 [256, 32768], P('depth', ('row', 'col'))
The draws below stay inside these ranges and needn't reach their ends.
Inputs may be any that keep to these rules, and one draw needn't show every extreme that they name: `cols1`: in each of the 256 block rows the 32 entries name different block columns, and for every g the entries g * 8 to g * 8 + 7 lie among block columns g * 64 to g * 64 + 63. `cols2`: in each of the 256 block rows the 32 entries name different block columns, and for every g the entries g * 8 to g * 8 + 7 lie among block columns g * 64 to g * 64 + 63.
All inputs are finite; a program needn't handle non-finite values. No bound on the sum of `act_mask` or of `mask2` on one device may be relied on, other than what follows from the above.
Results may differ from the reference program's by a relative error of at most 0.0047.
Values may be sent and summed in bfloat16 or wider, within the bound.
No kernel may reach another device: no remote copies, remote signals or barrier semaphores. Data moves between devices by JAX's collectives and lax.ppermute only.
A program may use at most 128 MiB of HBM per device.

```python
import jax
import jax.numpy as jnp
from jax import lax

N = 32768
BS = 128
K = 32
NB = 256
NB_COL = 64
NB_ROW = 64
KC = 8
KR = 8
M = 256


def pattern(key, extent, per_group):
    groups = NB // extent
    score_values = jax.random.randint(key, (NB, groups, extent), 0, 1 << 20, dtype=jnp.int32)
    score_values = score_values * extent + jnp.arange(extent, dtype=jnp.int32)
    ranked = jnp.argsort(score_values, axis=-1)[:, :, :per_group].astype(jnp.int32)
    placed = ranked + (jnp.arange(groups, dtype=jnp.int32) * extent)[None, :, None]
    return placed.reshape(NB, groups * per_group).astype(jnp.int32)


def draw_cols1(key, part):
    return pattern(jax.random.fold_in(key, 1), NB_COL, KC)


def draw_cols2(key, part):
    return pattern(jax.random.fold_in(key, 2), NB_ROW, KR)


def with_ends(entries, own_key, smallest, high):
    index_at = [jax.random.randint(jax.random.fold_in(own_key, axis), (), 0, length) for axis, length in enumerate(entries.shape)]
    longest = entries.shape.index(max(entries.shape))
    neighbour = index_at[:longest] + [(index_at[longest] + 1) % entries.shape[longest]] + index_at[longest + 1:]
    return entries.at[tuple(index_at)].set(smallest).at[tuple(neighbour)].set(high)


def level_of(stream_key, shape, cuts, low, high):
    level = 1.0
    for position, blocks in cuts:
        draws = jax.random.uniform(jax.random.fold_in(jax.random.fold_in(stream_key, 6), position), (blocks,), jnp.float32, low / len(cuts), high / len(cuts))
        level = level * jnp.repeat(jnp.exp(draws), shape[position] // blocks).reshape((-1,) + (1,) * (len(shape) - 1 - position))
    return level


def normal_values(rng, shape, scale, most, pieces=(), kind=jnp.bfloat16):
    drawn = jax.random.normal(rng, shape, jnp.float32) * scale
    if len(pieces) > 0:
        drawn = level_of(rng, shape, pieces, -0.22, 0.18) * drawn
    return jnp.clip(drawn, min=-most, max=most).astype(kind)


def setup_inputs(seed: int = 0) -> dict:
    arg_keys = jax.random.split(jax.random.key(seed), 10)
    return {
        "acts": normal_values(arg_keys[0], (M, N), 1.0, 6.0, ((0, 2), (1, 4))),
        "act_mask": with_ends((jax.random.randint(arg_keys[1], (M, NB), 0, 4) < 3).astype(jnp.int32), jax.random.fold_in(arg_keys[1], 1), 0, 1),
        "w1": normal_values(arg_keys[2], (NB, K, BS, BS), (K * BS) ** -0.5, 0.09375, ((0, 8), (1, 4))),
        "cols1": draw_cols1(jax.random.fold_in(arg_keys[9], 71), 0),
        "bias1": normal_values(arg_keys[4], (N,), 0.5, 3.0, ((0, 4),), jnp.float32),
        "mask2": with_ends((jax.random.randint(arg_keys[5], (M, NB), 0, 4) < 3).astype(jnp.int32), jax.random.fold_in(arg_keys[5], 1), 0, 1),
        "w2": normal_values(arg_keys[6], (NB, K, BS, BS), (K * BS // 4) ** -0.5, 0.1875, ((0, 8), (1, 4))),
        "cols2": draw_cols2(jax.random.fold_in(arg_keys[9], 71), 0),
        "bias2": normal_values(arg_keys[8], (N,), 0.5, 3.0, ((0, 16),), jnp.float32),
    }


def dense_layer(inputs, weights, targets, bias):
    blocks_in = inputs.reshape(M, NB, BS).astype(jnp.float32)

    def advance(running_total, block_row):
        incoming_rows = blocks_in[:, block_row]
        tiles = weights[block_row].astype(jnp.float32)
        product = jnp.einsum("mb,kbc->mkc", incoming_rows, tiles)
        return running_total.at[:, targets[block_row]].add(product), None

    start_value = jnp.zeros((M, NB, BS), jnp.float32)
    summed, unused = lax.scan(advance, start_value, jnp.arange(NB, dtype=jnp.int32))
    return jnp.maximum(summed + bias.reshape(NB, BS), 0.0)


def reference(acts, act_mask, w1, cols1, bias1, mask2, w2, cols2, bias2):
    masked = acts.reshape(M, NB, BS) * act_mask[:, :, None].astype(jnp.bfloat16)
    masked = masked.reshape(M, N)
    first = dense_layer(masked, w1, cols1, bias1)
    hidden = (first * mask2[:, :, None].astype(jnp.float32)).astype(jnp.bfloat16)
    second = dense_layer(hidden.reshape(M, N), w2, cols2, bias2)
    return second.astype(jnp.bfloat16).reshape(M, N)
```

```python
import functools

import jax
import jax.numpy as jnp
import numpy as np
from jax import lax
from jax.experimental import pallas as pl
from jax.experimental.pallas import tpu as pltpu
from jax.sharding import PartitionSpec as P


STEP = 4


def fold_kernel(low, parts, first_ref, place_ref, *refs):
    x_refs, (w_ref, *outs, acc) = refs[:parts], refs[parts:]
    step = pl.program_id(0)
    steps = pl.num_programs(0)
    stride, entries, block, _ = w_ref.shape

    @pl.when(step == 0)
    def _():
        acc[...] = jnp.zeros_like(acc)

    base = lax.rem(step + first_ref[0], steps) * stride
    for i in range(stride):
        if parts == 1:
            x = x_refs[0][:, i * block:(i + 1) * block]
        else:
            x = jnp.where(step < steps // 2, x_refs[0][i], x_refs[1][i])
        for k in range(0, entries, 2):
            pair = jnp.concatenate([w_ref[i, k], w_ref[i, k + 1]], axis=1)
            product = jnp.dot(x, pair, preferred_element_type=jnp.float32)
            for half in range(2):
                to = place_ref[(base + i) * entries + k + half]
                acc[to] = acc[to] + product[:, half * block:(half + 1) * block]

    @pl.when(step == steps - 1)
    def _():
        if low:
            outs[0][...] = acc[:low].astype(jnp.bfloat16)
        if low < acc.shape[0]:
            outs[-1][...] = acc[low:]


def fold(xs, weights, places, first, blocks, low):
    rows_in, entries, block, _ = weights.shape
    stride = min(STEP, rows_in)
    steps = rows_in // stride
    if len(xs) == 1:
        rows = xs[0].shape[0]
        x_specs = [pl.BlockSpec((rows, stride * block), lambda s, f, p: (0, s))]
    else:
        rows = xs[0].shape[1]
        last = steps // 2 - 1
        x_specs = [
            pl.BlockSpec((stride, rows, block), lambda s, f, p: (jnp.minimum(s, last), 0, 0)),
            pl.BlockSpec((stride, rows, block), lambda s, f, p: (jnp.maximum(s - last - 1, 0), 0, 0)),
        ]
    w_spec = pl.BlockSpec((stride, entries, block, block), lambda s, f, p: (lax.rem(s + f[0], steps), 0, 0, 0))
    shapes = []
    if low:
        shapes.append(jax.ShapeDtypeStruct((low, rows, block), jnp.bfloat16))
    if low < blocks:
        shapes.append(jax.ShapeDtypeStruct((blocks - low, rows, block), jnp.float32))
    return pl.pallas_call(
        functools.partial(fold_kernel, low, len(xs)),
        out_shape=shapes,
        grid_spec=pltpu.PrefetchScalarGridSpec(
            num_scalar_prefetch=2,
            grid=(steps,),
            in_specs=x_specs + [w_spec],
            out_specs=[pl.BlockSpec(s.shape, lambda s, f, p: (0, 0, 0)) for s in shapes],
            scratch_shapes=[pltpu.VMEM((blocks, rows, block), jnp.float32)],
        ),
        cost_estimate=pl.CostEstimate(
            flops=2 * rows * rows_in * entries * block * block,
            bytes_accessed=2 * weights.size,
            transcendentals=0,
        ),
    )(first.reshape(1), places.reshape(-1), *xs, weights)


def line_orders(size):
    order, right, left = [], [], []
    for place in range(size):
        sends = []
        for step in range(size - 1):
            up = place + size - 1 - step
            if place < up < size:
                sends.append((step, 0, up))
            down = place - size + 1 + step
            if 0 <= down < place:
                sends.append((step, 1, down))
        chunks = [s[2] for s in sends] + [place]
        order.append(chunks)
        right.append([next((i for i, s in enumerate(sends) if s[:2] == (step, 0)), 0) for step in range(size - 1)])
        left.append([next((i for i, s in enumerate(sends) if s[:2] == (step, 1)), 0) for step in range(size - 1)])
    slots = np.argsort(np.array(order), axis=1)
    return slots.astype(np.int32), np.array(right, np.int32), np.array(left, np.int32)


def exchange_plan(acts, act_mask, w1, cols1, bias1, mask2, w2, cols2, bias2):
    bf16, f32 = jnp.bfloat16, jnp.float32
    block = w1.shape[-1]
    rows = acts.shape[0]
    row_blocks = act_mask.shape[1]
    col_blocks = mask2.shape[1]
    half_in = row_blocks // 2
    half_mid = col_blocks // 2
    quarter = col_blocks // 4
    size_row, size_col = lax.axis_size("row"), lax.axis_size("col")
    r, c, d = lax.axis_index("row"), lax.axis_index("col"), lax.axis_index("depth")
    core = lax.rem(r, 2)
    over_depth = functools.partial(lax.ppermute, axis_name="depth", perm=[(0, 1), (1, 0)])
    over_core = functools.partial(lax.ppermute, axis_name="row", perm=[(i, i ^ 1) for i in range(size_row)])
    over_x = functools.partial(lax.ppermute, axis_name="row", perm=[(i, i ^ 2) for i in range(size_row)])

    live = act_mask.astype(bf16)

    def masked_half(which):
        a = lax.dynamic_slice_in_dim(acts, which * half_in * block, half_in * block, 1)
        m = lax.dynamic_slice_in_dim(live, which * half_in, half_in, 1)
        return (a.reshape(rows, half_in, block) * m[:, :, None]).reshape(rows, half_in * block)

    other_x = over_depth(masked_half(1 - d))
    own_x = masked_half(d)
    mask_own = lax.dynamic_slice_in_dim(mask2, d * half_mid + core * quarter, quarter, 1).astype(bf16)
    mask_other = over_depth(
        lax.dynamic_slice_in_dim(mask2, (1 - d) * half_mid + core * quarter, quarter, 1).astype(bf16)
    )

    to1 = lax.dynamic_slice_in_dim(cols1, d * half_in, half_in, 0) - c * col_blocks
    to_depth = to1 // half_mid
    to_core = (to1 // quarter) % 2
    same_core = 1 - (to_core ^ core)
    same_depth = 1 - (to_depth ^ d)
    place1 = same_core * half_mid + same_depth * quarter + to1 % quarter
    zero = jnp.int32(0)

    def layer1(x):
        low, high = fold([x], w1, place1, zero, col_blocks, half_mid)
        return high + over_core(low).astype(f32)

    sum_own = layer1(own_x)
    got_other = over_depth(sum_own[:quarter].astype(bf16))
    sum_other = layer1(other_x)
    got_own = over_depth(sum_other[:quarter].astype(bf16))
    bias_blocks = lax.dynamic_slice_in_dim(
        bias1.reshape(col_blocks, 1, block), d * half_mid + core * quarter, quarter, 0
    )

    def hidden(summed, got, mask):
        part = summed[quarter:] + got.astype(f32)
        z1 = part + over_x(part.astype(bf16)).astype(f32)
        out = (jnp.maximum(z1 + bias_blocks, 0.0) * mask.astype(f32).T[:, :, None]).astype(bf16)
        return out, over_core(out)

    hidden_other = hidden(sum_other, got_other, mask_other)
    hidden_own = hidden(sum_own, got_own, mask_own)

    slots, right, left = (jnp.asarray(t) for t in line_orders(size_col))
    to2 = lax.dynamic_slice_in_dim(cols2, d * half_mid, half_mid, 0) - r * row_blocks
    share = row_blocks // size_col
    my_slots = lax.dynamic_index_in_dim(slots, c, 0, keepdims=False)
    chunk = to2 // share
    slot = sum(jnp.where(chunk == i, my_slots[i], 0) for i in range(size_col))
    place2 = slot * share + to2 % share
    first = core * (w2.shape[0] // min(STEP, w2.shape[0]) // 2)
    (for_other,) = fold(hidden_other, w2, place2, first, row_blocks, row_blocks)
    from_other = [over_depth(for_other[i * share:(i + 1) * share]) for i in range(size_col)]
    (mine,) = fold(hidden_own, w2, place2, first, row_blocks, 0)
    total = [mine[i * share:(i + 1) * share] + from_other[i].astype(f32) for i in range(size_col)]

    my_right = lax.dynamic_index_in_dim(right, c, 0, keepdims=False)
    my_left = lax.dynamic_index_in_dim(left, c, 0, keepdims=False)
    up = down = None
    for step in range(size_col - 1):

        def send(pick, got):
            value = total[0]
            for i in range(1, min(step + 1, size_col - 1)):
                value = jnp.where(pick == i, total[i], value)
            if step >= 1:
                value = jnp.where(pick == step, total[step], value)
            return value if got is None else value + got.astype(f32)

        go_up = send(my_right[step], up).astype(bf16)
        go_down = send(my_left[step], down).astype(bf16)
        up = lax.ppermute(go_up, "col", [(i, i + 1) for i in range(step + 1)])
        down = lax.ppermute(go_down, "col", [(size_col - 1 - i, size_col - 2 - i) for i in range(step + 1)])
    outcome = total[-1] + up.astype(f32) + down.astype(f32)
    outcome = jnp.maximum(outcome + bias2.reshape(share, 1, block), 0.0).astype(bf16)
    return outcome.transpose(1, 0, 2).reshape(rows, -1)


def fold_function(inputs, targets, stride):

    def add_tiles(running_total, tiles):

        def advance(number, total):
            offset = number * stride
            block_list = lax.dynamic_slice_in_dim(tiles, offset, stride, 0)
            incoming_rows = lax.dynamic_slice_in_dim(inputs, offset, stride, 1)
            wanted = lax.dynamic_slice_in_dim(targets, offset, stride, 0)
            product = jnp.einsum(
                "tws,wish->twih", incoming_rows, block_list, preferred_element_type=jnp.float32
            )
            flat_product = product.reshape(product.shape[0], -1, product.shape[-1])
            return total.at[:, wanted.reshape(-1)].add(flat_product)

        return lax.fori_loop(0, tiles.shape[0] // stride, advance, running_total)

    return add_tiles


def gather_plan(acts, act_mask, w1, cols1, bias1, mask2, w2, cols2, bias2):
    block = w1.shape[-1]
    rows_dev = acts.shape[0]
    row_blocks = act_mask.shape[1]
    col_blocks = mask2.shape[1]
    row_index = lax.axis_index("row")
    col_index = lax.axis_index("col")
    masked = acts.reshape(rows_dev, row_blocks, block) * act_mask[:, :, None].astype(jnp.bfloat16)
    first_targets = cols1 - col_index * col_blocks
    second_targets = cols2 - row_index * row_blocks
    first_fold = fold_function(masked, first_targets, w1.shape[0])
    first_sum = first_fold(
        jnp.zeros((rows_dev, col_blocks, block), jnp.float32), lax.all_gather(w1, "depth", axis=0, tiled=True)
    )
    bias_blocks = bias1.reshape(col_blocks, block)
    share = col_blocks // lax.axis_size("row")
    part_sum = lax.psum_scatter(first_sum, "row", scatter_dimension=1, tiled=True)
    bias_part = lax.dynamic_slice_in_dim(bias_blocks, row_index * share, share, 0)
    mask_part = lax.dynamic_slice_in_dim(mask2, row_index * share, share, 1)
    hidden_part = jnp.maximum(part_sum + bias_part, 0.0) * mask_part[:, :, None].astype(jnp.float32)
    hidden = lax.all_gather(hidden_part.astype(jnp.bfloat16), "row", axis=1, tiled=True)
    second_fold = fold_function(hidden, second_targets, w2.shape[0])
    second_sum = second_fold(
        jnp.zeros((rows_dev, row_blocks, block), jnp.float32), lax.all_gather(w2, "depth", axis=0, tiled=True)
    )
    outcome = lax.psum_scatter(second_sum, "col", scatter_dimension=1, tiled=True)
    bias_out = bias2.reshape(outcome.shape[1], block)
    return jnp.maximum(outcome + bias_out, 0.0).astype(jnp.bfloat16).reshape(rows_dev, -1)


def solution(mesh):
    sizes = dict(mesh.shape)
    pairs = sizes["depth"] == 2 and sizes["row"] == 4
    return jax.shard_map(
        exchange_plan if pairs else gather_plan,
        mesh=mesh,
        in_specs=(
            P("depth", "row"),
            P("depth", "row"),
            P(("row", "depth"), "col", None, None),
            P("row", "col"),
            P("col"),
            P("depth", "col"),
            P(("col", "depth"), "row", None, None),
            P("col", "row"),
            P(("row", "col")),
        ),
        out_specs=P("depth", ("row", "col")),
        check_vma=False,
    )
```

```python
import functools

import jax
import jax.numpy as jnp
import numpy as np
from jax import lax
from jax.experimental import pallas as pl
from jax.experimental.pallas import tpu as pltpu
from jax.sharding import PartitionSpec as P


UNROLL = 4
VMEM_LIMIT = 8 * 1024 * 1024


def mask_kernel(half_ref, acts_ref, live_ref, out_ref):
    blocks, _, block = out_ref.shape
    live = live_ref[...].astype(jnp.float32).T
    for i in range(blocks):
        x = acts_ref[:, i * block:(i + 1) * block].astype(jnp.float32)
        out_ref[i] = (x * live[:, i:i + 1]).astype(jnp.bfloat16)


def masked_half(acts, act_mask, half):
    rows, width = acts.shape
    blocks = act_mask.shape[1] // 2
    block = width // act_mask.shape[1]
    steps = 2
    return pl.pallas_call(
        mask_kernel,
        out_shape=pltpu.VMEM((blocks, rows, block), jnp.bfloat16),
        grid_spec=pltpu.PrefetchScalarGridSpec(
            num_scalar_prefetch=1,
            grid=(steps,),
            in_specs=[
                pl.BlockSpec((rows, width // 2 // steps), lambda s, h: (0, h[0] * steps + s)),
                pl.BlockSpec((blocks // steps, rows), lambda s, h: (h[0] * steps + s, 0)),
            ],
            out_specs=pl.BlockSpec((blocks // steps, rows, block), lambda s, h: (s, 0, 0)),
        ),
        compiler_params=pltpu.CompilerParams(vmem_limit_bytes=VMEM_LIMIT),
        cost_estimate=pl.CostEstimate(flops=rows * width, bytes_accessed=2 * rows * width, transcendentals=0),
    )(half.reshape(1), pltpu.with_memory_space_constraint(acts, pltpu.HBM), act_mask.T)


def clear(acc):

    def body(i, carry):
        acc[i] = jnp.zeros_like(acc[i])
        return carry

    lax.fori_loop(0, acc.shape[0], body, 0, unroll=4)


def add_products(acc, x_ref, w_ref, place_ref, start, first, count):
    _, entries, block, _ = w_ref.shape

    def advance(step, carry):
        for i in range(UNROLL):
            at = first + step * UNROLL + i
            row = start + at
            x = x_ref[at]
            for k in range(0, entries, 2):
                pair = jnp.concatenate([w_ref[row, k], w_ref[row, k + 1]], axis=1)
                product = jnp.dot(x, pair, preferred_element_type=jnp.float32)
                for half in range(2):
                    to = place_ref[row * entries + k + half]
                    acc[to] = acc[to] + product[:, half * block:(half + 1) * block]
        return carry

    lax.fori_loop(0, count // UNROLL, advance, 0)


def write_out(acc, outs):
    start = 0
    for out in outs:

        def body(i, carry, out=out, start=start):
            out[i] = acc[start + i].astype(out.dtype)
            return carry

        lax.fori_loop(0, out.shape[0], body, 0, unroll=4)
        start += out.shape[0]


def fold_kernel(parts, load, starts_ref, place_ref, *refs):
    x_refs, w_ref, refs = refs[:parts], refs[parts], refs[parts + 1:]
    copies = []
    if load:
        *refs, sems = refs
        *outs, keep_ref, acc = refs
        for part, x_ref in enumerate(x_refs):
            for first in range(0, x_ref.shape[0], UNROLL):
                rows = pl.ds(starts_ref[part] + first, UNROLL)
                copies.append(pltpu.make_async_copy(w_ref.at[rows], keep_ref.at[rows], sems.at[len(copies)]))
        w_ref = keep_ref
    else:
        *outs, acc = refs
    for copy in copies:
        copy.start()
    clear(acc)
    for part, x_ref in enumerate(x_refs):
        if load:
            for first in range(0, x_ref.shape[0], UNROLL):
                copies.pop(0).wait()
                add_products(acc, x_ref, w_ref, place_ref, starts_ref[part], first, UNROLL)
        else:
            add_products(acc, x_ref, w_ref, place_ref, starts_ref[part], 0, x_ref.shape[0])
    write_out(acc, outs)


def fold(xs, weights, places, starts, segments, load=False):
    rows_in, entries, block, _ = weights.shape
    rows = xs[0].shape[1]
    total = sum(count for count, _ in segments)
    smem = pl.BlockSpec(memory_space=pltpu.SMEM)
    vmem = pl.BlockSpec(memory_space=pltpu.VMEM)
    hbm = pl.BlockSpec(memory_space=pltpu.HBM)
    in_vmem = functools.partial(pltpu.with_memory_space_constraint, memory_space=pltpu.VMEM)
    in_hbm = functools.partial(pltpu.with_memory_space_constraint, memory_space=pltpu.HBM)
    out_shape = [pltpu.VMEM((count, rows, block), kind) for count, kind in segments]
    scratch = [pltpu.VMEM((total, rows, block), jnp.float32)]
    if load:
        out_shape.append(pltpu.VMEM(weights.shape, weights.dtype))
        scratch.append(pltpu.SemaphoreType.DMA((rows_in // UNROLL,)))
    elif len(segments) == 1:
        scratch = []
    return pl.pallas_call(
        functools.partial(fold_kernel, len(xs), load),
        out_shape=out_shape,
        in_specs=[smem, smem] + [vmem] * len(xs) + [hbm if load else vmem],
        out_specs=[vmem] * len(out_shape),
        scratch_shapes=scratch,
        compiler_params=pltpu.CompilerParams(vmem_limit_bytes=VMEM_LIMIT),
        cost_estimate=pl.CostEstimate(
            flops=2 * rows * rows_in * entries * block * block,
            bytes_accessed=2 * weights.size,
            transcendentals=0,
        ),
    )(jnp.stack(starts), places.reshape(-1), *map(in_vmem, xs), (in_hbm if load else in_vmem)(weights))


def finish_kernel(own_ref, up_ref, down_ref, bias_ref, out_ref):
    share, _, block = own_ref.shape
    for i in range(share):
        total = own_ref[i] + up_ref[i].astype(jnp.float32) + down_ref[i].astype(jnp.float32)
        out_ref[:, i * block:(i + 1) * block] = jnp.maximum(total + bias_ref[i:i + 1, :], 0.0).astype(jnp.bfloat16)


def line_orders(size):
    order, right, left = [], [], []
    for place in range(size):
        sends = []
        for step in range(size - 1):
            up = place + size - 1 - step
            if place < up < size:
                sends.append((step, 0, up))
            down = place - size + 1 + step
            if 0 <= down < place:
                sends.append((step, 1, down))
        chunks = [s[2] for s in sends] + [place]
        order.append(chunks)
        right.append([next((i for i, s in enumerate(sends) if s[:2] == (step, 0)), 0) for step in range(size - 1)])
        left.append([next((i for i, s in enumerate(sends) if s[:2] == (step, 1)), 0) for step in range(size - 1)])
    slots = np.argsort(np.array(order), axis=1)
    return slots.astype(np.int32), np.array(right, np.int32), np.array(left, np.int32)


def exchange_plan(acts, act_mask, w1, cols1, bias1, mask2, w2, cols2, bias2):
    bf16, f32 = jnp.bfloat16, jnp.float32
    block = w1.shape[-1]
    rows = acts.shape[0]
    row_blocks = act_mask.shape[1]
    col_blocks = mask2.shape[1]
    half_in = row_blocks // 2
    half_mid = col_blocks // 2
    quarter = col_blocks // 4
    size_row, size_col = lax.axis_size("row"), lax.axis_size("col")
    r, c, d = lax.axis_index("row"), lax.axis_index("col"), lax.axis_index("depth")
    core = lax.rem(r, 2)
    over_depth = functools.partial(lax.ppermute, axis_name="depth", perm=[(0, 1), (1, 0)])
    over_core = functools.partial(lax.ppermute, axis_name="row", perm=[(i, i ^ 1) for i in range(size_row)])
    over_x = functools.partial(lax.ppermute, axis_name="row", perm=[(i, i ^ 2) for i in range(size_row)])
    zero = jnp.int32(0)

    other_x = over_depth(masked_half(acts, act_mask, 1 - d))
    own_x = masked_half(acts, act_mask, d)
    mask_own = lax.dynamic_slice_in_dim(mask2, d * half_mid + core * quarter, quarter, 1).astype(bf16)
    mask_other = over_depth(
        lax.dynamic_slice_in_dim(mask2, (1 - d) * half_mid + core * quarter, quarter, 1).astype(bf16)
    )
    bias_blocks = lax.dynamic_slice_in_dim(
        bias1.reshape(col_blocks, 1, block), d * half_mid + core * quarter, quarter, 0
    )

    to1 = lax.dynamic_slice_in_dim(cols1, d * half_in, half_in, 0) - c * col_blocks
    to_depth = to1 // half_mid
    to_core = (to1 // quarter) % 2
    same_core = 1 - (to_core ^ core)
    same_depth = 1 - (to_depth ^ d)
    place1 = same_core * half_mid + same_depth * quarter + to1 % quarter

    slots, right, left = line_orders(size_col)

    def mine_of(table):
        return sum(jnp.where(c == i, int(v), 0) for i, v in enumerate(table))

    to2 = lax.dynamic_slice_in_dim(cols2, d * half_mid, half_mid, 0) - r * row_blocks
    share = row_blocks // size_col
    chunk = to2 // share
    slot = sum(jnp.where(chunk == i, mine_of(slots[:, i]), 0) for i in range(size_col))
    place2 = slot * share + to2 % share
    own_x, mask_other, place1, place2 = lax.optimization_barrier((own_x, mask_other, place1, place2))

    segments = [(half_mid, bf16), (quarter, f32), (quarter, f32)]

    def core_sums(low, send, keep):
        low = over_core(low)
        return (send + low[:quarter].astype(f32)).astype(bf16), keep + low[quarter:].astype(f32)

    *sums, w1 = fold([own_x], w1, place1, [zero], segments, load=True)
    send_own, keep_own = core_sums(*sums)
    got_other = over_depth(send_own)
    sums = fold([other_x], w1, place1, [zero], segments)
    send_other, keep_other = core_sums(*sums)
    got_own = over_depth(send_other)

    def hidden(keep, got, mask):
        part = keep + got.astype(f32)
        z1 = part + over_x(part.astype(bf16)).astype(f32)
        out = (jnp.maximum(z1 + bias_blocks, 0.0) * mask.astype(f32).T[:, :, None]).astype(bf16)
        return [out, over_core(out)]

    hidden_other = hidden(keep_other, got_other, mask_other)
    hidden_own = hidden(keep_own, got_own, mask_own)
    starts = [core * quarter, (1 - core) * quarter]
    *for_other, w2 = fold(hidden_other, w2, place2, starts, [(share, bf16)] * size_col, load=True)
    from_other = [over_depth(part) for part in for_other]
    (mine,) = fold(hidden_own, w2, place2, starts, [(row_blocks, f32)])
    total = [mine[i * share:(i + 1) * share] + f.astype(f32) for i, f in enumerate(from_other)]

    up = down = None
    for step in range(size_col - 1):

        def send(table, got):
            pick = mine_of(table[:, step])
            value = total[0]
            for i in range(1, step + 1):
                value = jnp.where(pick == i, total[i], value)
            return (value if got is None else value + got.astype(f32)).astype(bf16)

        go_up, go_down = send(right, up), send(left, down)
        up = lax.ppermute(go_up, "col", [(i, i + 1) for i in range(step + 1)])
        down = lax.ppermute(go_down, "col", [(size_col - 1 - i, size_col - 2 - i) for i in range(step + 1)])
    return pl.pallas_call(
        finish_kernel,
        out_shape=jax.ShapeDtypeStruct((rows, share * block), bf16),
        compiler_params=pltpu.CompilerParams(vmem_limit_bytes=VMEM_LIMIT),
    )(total[-1], up, down, bias2.reshape(share, block))


def fold_function(inputs, targets, stride):

    def add_tiles(running_total, tiles):

        def advance(number, total):
            offset = number * stride
            block_list = lax.dynamic_slice_in_dim(tiles, offset, stride, 0)
            incoming_rows = lax.dynamic_slice_in_dim(inputs, offset, stride, 1)
            wanted = lax.dynamic_slice_in_dim(targets, offset, stride, 0)
            product = jnp.einsum(
                "tws,wish->twih", incoming_rows, block_list, preferred_element_type=jnp.float32
            )
            flat_product = product.reshape(product.shape[0], -1, product.shape[-1])
            return total.at[:, wanted.reshape(-1)].add(flat_product)

        return lax.fori_loop(0, tiles.shape[0] // stride, advance, running_total)

    return add_tiles


def gather_plan(acts, act_mask, w1, cols1, bias1, mask2, w2, cols2, bias2):
    block = w1.shape[-1]
    rows_dev = acts.shape[0]
    row_blocks = act_mask.shape[1]
    col_blocks = mask2.shape[1]
    row_index = lax.axis_index("row")
    col_index = lax.axis_index("col")
    masked = acts.reshape(rows_dev, row_blocks, block) * act_mask[:, :, None].astype(jnp.bfloat16)
    first_targets = cols1 - col_index * col_blocks
    second_targets = cols2 - row_index * row_blocks
    first_fold = fold_function(masked, first_targets, w1.shape[0])
    first_sum = first_fold(
        jnp.zeros((rows_dev, col_blocks, block), jnp.float32), lax.all_gather(w1, "depth", axis=0, tiled=True)
    )
    bias_blocks = bias1.reshape(col_blocks, block)
    share = col_blocks // lax.axis_size("row")
    part_sum = lax.psum_scatter(first_sum, "row", scatter_dimension=1, tiled=True)
    bias_part = lax.dynamic_slice_in_dim(bias_blocks, row_index * share, share, 0)
    mask_part = lax.dynamic_slice_in_dim(mask2, row_index * share, share, 1)
    hidden_part = jnp.maximum(part_sum + bias_part, 0.0) * mask_part[:, :, None].astype(jnp.float32)
    hidden = lax.all_gather(hidden_part.astype(jnp.bfloat16), "row", axis=1, tiled=True)
    second_fold = fold_function(hidden, second_targets, w2.shape[0])
    second_sum = second_fold(
        jnp.zeros((rows_dev, row_blocks, block), jnp.float32), lax.all_gather(w2, "depth", axis=0, tiled=True)
    )
    outcome = lax.psum_scatter(second_sum, "col", scatter_dimension=1, tiled=True)
    bias_out = bias2.reshape(outcome.shape[1], block)
    return jnp.maximum(outcome + bias_out, 0.0).astype(jnp.bfloat16).reshape(rows_dev, -1)


def solution(mesh):
    sizes = dict(mesh.shape)
    pairs = sizes["depth"] == 2 and sizes["row"] == 4
    return jax.shard_map(
        exchange_plan if pairs else gather_plan,
        mesh=mesh,
        in_specs=(
            P("depth", "row"),
            P("depth", "row"),
            P(("row", "depth"), "col", None, None),
            P("row", "col"),
            P("col"),
            P("depth", "col"),
            P(("col", "depth"), "row", None, None),
            P("col", "row"),
            P(("row", "col")),
        ),
        out_specs=P("depth", ("row", "col")),
        check_vma=False,
    )
```

```python
import functools

import jax
import jax.numpy as jnp
from jax import lax
from jax.experimental import pallas as pl
from jax.experimental.pallas import tpu as pltpu
from jax.sharding import PartitionSpec as P


UNROLL = 4
VMEM_LIMIT = 8 * 1024 * 1024

in_vmem = functools.partial(pltpu.with_memory_space_constraint, memory_space=pltpu.VMEM)
in_hbm = functools.partial(pltpu.with_memory_space_constraint, memory_space=pltpu.HBM)


def mask_kernel(half_ref, acts_ref, live_ref, out_ref):
    blocks, _, block = out_ref.shape
    live = live_ref[...].astype(jnp.float32).T
    for i in range(blocks):
        x = acts_ref[:, i * block:(i + 1) * block].astype(jnp.float32)
        out_ref[i] = (x * live[:, i:i + 1]).astype(jnp.bfloat16)


def masked_half(acts, act_mask, half):
    rows, width = acts.shape
    blocks = act_mask.shape[1] // 2
    block = width // act_mask.shape[1]
    steps = 2
    return pl.pallas_call(
        mask_kernel,
        out_shape=pltpu.VMEM((blocks, rows, block), jnp.bfloat16),
        grid_spec=pltpu.PrefetchScalarGridSpec(
            num_scalar_prefetch=1,
            grid=(steps,),
            in_specs=[
                pl.BlockSpec((rows, width // 2 // steps), lambda s, h: (0, h[0] * steps + s)),
                pl.BlockSpec((blocks // steps, rows), lambda s, h: (h[0] * steps + s, 0)),
            ],
            out_specs=pl.BlockSpec((blocks // steps, rows, block), lambda s, h: (s, 0, 0)),
        ),
        compiler_params=pltpu.CompilerParams(vmem_limit_bytes=VMEM_LIMIT),
        cost_estimate=pl.CostEstimate(flops=rows * width, bytes_accessed=2 * rows * width, transcendentals=0),
    )(half.reshape(1), in_hbm(acts), in_hbm(act_mask.T))


def clear(acc):

    def body(i, carry):
        acc[i] = jnp.zeros_like(acc[i])
        return carry

    lax.fori_loop(0, acc.shape[0], body, 0, unroll=4)


def add_products(acc, x_ref, w_ref, place_ref, start, first, count):
    _, entries, block, _ = w_ref.shape

    def advance(step, carry):
        for i in range(UNROLL):
            at = first + step * UNROLL + i
            row = start + at
            x = x_ref[at]
            for k in range(0, entries, 2):
                pair = jnp.concatenate([w_ref[row, k], w_ref[row, k + 1]], axis=1)
                product = jnp.dot(x, pair, preferred_element_type=jnp.float32)
                for half in range(2):
                    to = place_ref[row * entries + k + half]
                    acc[to] = acc[to] + product[:, half * block:(half + 1) * block]
        return carry

    lax.fori_loop(0, count // UNROLL, advance, 0)


def write_out(acc, outs):
    start = 0
    for out in outs:

        def body(i, carry, out=out, start=start):
            out[i] = acc[start + i].astype(out.dtype)
            return carry

        lax.fori_loop(0, out.shape[0], body, 0, unroll=4)
        start += out.shape[0]


def fold_kernel(parts, load, starts_ref, place_ref, *refs):
    x_refs, w_ref, refs = refs[:parts], refs[parts], refs[parts + 1:]
    copies = []
    if load:
        *refs, sems = refs
        *outs, keep_ref, acc = refs
        for part, x_ref in enumerate(x_refs):
            for first in range(0, x_ref.shape[0], UNROLL):
                rows = pl.ds(starts_ref[part] + first, UNROLL)
                copies.append(pltpu.make_async_copy(w_ref.at[rows], keep_ref.at[rows], sems.at[len(copies)]))
        w_ref = keep_ref
    else:
        *outs, acc = refs
    for copy in copies:
        copy.start()
    clear(acc)
    for part, x_ref in enumerate(x_refs):
        if load:
            for first in range(0, x_ref.shape[0], UNROLL):
                copies.pop(0).wait()
                add_products(acc, x_ref, w_ref, place_ref, starts_ref[part], first, UNROLL)
        else:
            add_products(acc, x_ref, w_ref, place_ref, starts_ref[part], 0, x_ref.shape[0])
    write_out(acc, outs)


def fold(xs, weights, places, starts, segments, load=False):
    rows_in, entries, block, _ = weights.shape
    rows = xs[0].shape[1]
    total = sum(count for count, _ in segments)
    smem = pl.BlockSpec(memory_space=pltpu.SMEM)
    vmem = pl.BlockSpec(memory_space=pltpu.VMEM)
    hbm = pl.BlockSpec(memory_space=pltpu.HBM)
    out_shape = [pltpu.VMEM((count, rows, block), kind) for count, kind in segments]
    scratch = [pltpu.VMEM((total, rows, block), jnp.float32)]
    if load:
        out_shape.append(pltpu.VMEM(weights.shape, weights.dtype))
        scratch.append(pltpu.SemaphoreType.DMA((rows_in // UNROLL,)))
    elif len(segments) == 1:
        scratch = []
    return pl.pallas_call(
        functools.partial(fold_kernel, len(xs), load),
        out_shape=out_shape,
        in_specs=[smem, smem] + [vmem] * len(xs) + [hbm if load else vmem],
        out_specs=[vmem] * len(out_shape),
        scratch_shapes=scratch,
        compiler_params=pltpu.CompilerParams(vmem_limit_bytes=VMEM_LIMIT),
        cost_estimate=pl.CostEstimate(
            flops=2 * rows * rows_in * entries * block * block,
            bytes_accessed=2 * weights.size,
            transcendentals=0,
        ),
    )(jnp.stack(starts), places.reshape(-1), *map(in_vmem, xs), (in_hbm if load else in_vmem)(weights))


def add_kernel(*refs):
    *parts, out_ref = refs

    def body(i, carry):
        total = parts[0][i]
        for part in parts[1:]:
            total = total + part[i].astype(jnp.float32)
        out_ref[i] = total.astype(jnp.bfloat16)
        return carry

    lax.fori_loop(0, out_ref.shape[0], body, 0, unroll=2)


def add(parts):
    vmem = pl.BlockSpec(memory_space=pltpu.VMEM)
    return pl.pallas_call(
        add_kernel,
        out_shape=pltpu.VMEM(parts[0].shape, jnp.bfloat16),
        in_specs=[vmem] * len(parts),
        out_specs=vmem,
        compiler_params=pltpu.CompilerParams(vmem_limit_bytes=VMEM_LIMIT),
    )(*map(in_vmem, parts))


def finish_kernel(*refs):
    *parts, bias_ref, out_ref = refs
    share, _, block = parts[0].shape
    for i in range(share):
        total = parts[0][i]
        for part in parts[1:]:
            total = total + part[i].astype(jnp.float32)
        total = jnp.maximum(total + bias_ref[i:i + 1, :], 0.0)
        out_ref[:, i * block:(i + 1) * block] = total.astype(jnp.bfloat16)


def exchange_plan(acts, act_mask, w1, cols1, bias1, mask2, w2, cols2, bias2):
    bf16, f32 = jnp.bfloat16, jnp.float32
    block = w1.shape[-1]
    rows = acts.shape[0]
    row_blocks = act_mask.shape[1]
    col_blocks = mask2.shape[1]
    half_in = row_blocks // 2
    half_mid = col_blocks // 2
    quarter = col_blocks // 4
    size_row, size_col = lax.axis_size("row"), lax.axis_size("col")
    r, c, d = lax.axis_index("row"), lax.axis_index("col"), lax.axis_index("depth")
    core = lax.rem(r, 2)
    over_depth = functools.partial(lax.ppermute, axis_name="depth", perm=[(0, 1), (1, 0)])
    over_core = functools.partial(lax.ppermute, axis_name="row", perm=[(i, i ^ 1) for i in range(size_row)])
    over_x = functools.partial(lax.ppermute, axis_name="row", perm=[(i, i ^ 2) for i in range(size_row)])
    zero = jnp.int32(0)

    other_x = over_depth(masked_half(acts, act_mask, 1 - d))
    own_x = masked_half(acts, act_mask, d)
    mask_own = lax.dynamic_slice_in_dim(mask2, d * half_mid + core * quarter, quarter, 1).astype(bf16)
    mask_other = over_depth(
        lax.dynamic_slice_in_dim(mask2, (1 - d) * half_mid + core * quarter, quarter, 1).astype(bf16)
    )
    bias_blocks = lax.dynamic_slice_in_dim(
        bias1.reshape(col_blocks, 1, block), d * half_mid + core * quarter, quarter, 0
    )

    to1 = lax.dynamic_slice_in_dim(cols1, d * half_in, half_in, 0) - c * col_blocks
    to_depth = to1 // half_mid
    to_core = (to1 // quarter) % 2
    same_core = 1 - (to_core ^ core)
    same_depth = 1 - (to_depth ^ d)
    place1 = same_core * half_mid + same_depth * quarter + to1 % quarter

    to2 = lax.dynamic_slice_in_dim(cols2, d * half_mid, half_mid, 0) - r * row_blocks
    share = row_blocks // size_col
    chunk = to2 // share
    far = jnp.where(c < size_col // 2, size_col - 1, 0)
    slot = jnp.where(chunk == far, 0, jnp.where(chunk == (far ^ 1), 1, jnp.where(chunk == (c ^ 1), 2, 3)))
    place2 = slot * share + to2 % share
    own_x, place1, place2 = lax.optimization_barrier((own_x, place1, place2))

    segments = [(half_mid, bf16), (quarter, f32), (quarter, f32)]

    def core_sums(low, send, keep):
        low = over_core(low)
        return lax.optimization_barrier(
            ((send + low[:quarter].astype(f32)).astype(bf16), keep + low[quarter:].astype(f32))
        )

    *sums, w1 = fold([own_x], w1, place1, [zero], segments, load=True)
    send_own, keep_own = core_sums(*sums)
    got_other = over_depth(send_own)
    sums = fold([other_x], w1, place1, [zero], segments)
    send_other, keep_other = core_sums(*sums)
    got_own = over_depth(send_other)

    def x_sums(keep, got):
        part = keep + got.astype(f32)
        part, low = lax.optimization_barrier((part, part.astype(bf16)))
        return part, over_x(low)

    def hidden(part, low, mask):
        z1 = part + low.astype(f32)
        out = (jnp.maximum(z1 + bias_blocks, 0.0) * mask.astype(f32).T[:, :, None]).astype(bf16)
        out = lax.optimization_barrier(out)
        return [out, over_core(out)]

    sums_other = x_sums(keep_other, got_other)
    sums_own = x_sums(keep_own, got_own)
    hidden_other = hidden(*sums_other, mask_other)
    starts = [core * quarter, (1 - core) * quarter]
    *for_other, w2 = fold(hidden_other, w2, place2, starts, [(share, bf16)] * size_col, load=True)
    got = []
    for part in for_other:
        got.append(over_depth(part))
    part_own, low_own, w2 = lax.optimization_barrier((*sums_own, w2))
    hidden_own = hidden(part_own, low_own, mask_own)
    mine = fold(hidden_own, w2, place2, starts, [(share, f32)] * size_col)

    over_col = functools.partial(lax.ppermute, axis_name="col")
    ends = [(0, 1), (3, 2)]
    ends0 = over_col(add([mine[0], got[0]]), perm=ends)
    ends1 = over_col(add([mine[1], got[1]]), perm=ends)
    cross0 = over_col(add([mine[0], got[0], ends0]), perm=[(1, 3), (2, 0)])
    near = over_col(add([mine[2], got[2]]), perm=[(i, i ^ 1) for i in range(size_col)])
    cross1 = over_col(add([mine[1], got[1], ends1]), perm=[(1, 2), (2, 1)])
    parts = [mine[3], got[3], cross0, near, cross1]
    return pl.pallas_call(
        finish_kernel,
        out_shape=jax.ShapeDtypeStruct((rows, share * block), bf16),
        compiler_params=pltpu.CompilerParams(vmem_limit_bytes=VMEM_LIMIT),
    )(*map(in_vmem, parts), bias2.reshape(share, block))


def fold_function(inputs, targets, stride):

    def add_tiles(running_total, tiles):

        def advance(number, total):
            offset = number * stride
            block_list = lax.dynamic_slice_in_dim(tiles, offset, stride, 0)
            incoming_rows = lax.dynamic_slice_in_dim(inputs, offset, stride, 1)
            wanted = lax.dynamic_slice_in_dim(targets, offset, stride, 0)
            product = jnp.einsum(
                "tws,wish->twih", incoming_rows, block_list, preferred_element_type=jnp.float32
            )
            flat_product = product.reshape(product.shape[0], -1, product.shape[-1])
            return total.at[:, wanted.reshape(-1)].add(flat_product)

        return lax.fori_loop(0, tiles.shape[0] // stride, advance, running_total)

    return add_tiles


def gather_plan(acts, act_mask, w1, cols1, bias1, mask2, w2, cols2, bias2):
    block = w1.shape[-1]
    rows_dev = acts.shape[0]
    row_blocks = act_mask.shape[1]
    col_blocks = mask2.shape[1]
    row_index = lax.axis_index("row")
    col_index = lax.axis_index("col")
    masked = acts.reshape(rows_dev, row_blocks, block) * act_mask[:, :, None].astype(jnp.bfloat16)
    first_targets = cols1 - col_index * col_blocks
    second_targets = cols2 - row_index * row_blocks
    first_fold = fold_function(masked, first_targets, w1.shape[0])
    first_sum = first_fold(
        jnp.zeros((rows_dev, col_blocks, block), jnp.float32), lax.all_gather(w1, "depth", axis=0, tiled=True)
    )
    bias_blocks = bias1.reshape(col_blocks, block)
    share = col_blocks // lax.axis_size("row")
    part_sum = lax.psum_scatter(first_sum, "row", scatter_dimension=1, tiled=True)
    bias_part = lax.dynamic_slice_in_dim(bias_blocks, row_index * share, share, 0)
    mask_part = lax.dynamic_slice_in_dim(mask2, row_index * share, share, 1)
    hidden_part = jnp.maximum(part_sum + bias_part, 0.0) * mask_part[:, :, None].astype(jnp.float32)
    hidden = lax.all_gather(hidden_part.astype(jnp.bfloat16), "row", axis=1, tiled=True)
    second_fold = fold_function(hidden, second_targets, w2.shape[0])
    second_sum = second_fold(
        jnp.zeros((rows_dev, row_blocks, block), jnp.float32), lax.all_gather(w2, "depth", axis=0, tiled=True)
    )
    outcome = lax.psum_scatter(second_sum, "col", scatter_dimension=1, tiled=True)
    bias_out = bias2.reshape(outcome.shape[1], block)
    return jnp.maximum(outcome + bias_out, 0.0).astype(jnp.bfloat16).reshape(rows_dev, -1)


def solution(mesh):
    sizes = dict(mesh.shape)
    pairs = sizes["depth"] == 2 and sizes["row"] == 4 and sizes["col"] == 4
    return jax.shard_map(
        exchange_plan if pairs else gather_plan,
        mesh=mesh,
        in_specs=(
            P("depth", "row"),
            P("depth", "row"),
            P(("row", "depth"), "col", None, None),
            P("row", "col"),
            P("col"),
            P("depth", "col"),
            P(("col", "depth"), "row", None, None),
            P("col", "row"),
            P(("row", "col")),
        ),
        out_specs=P("depth", ("row", "col")),
        check_vma=False,
    )
```

```python
import functools

import jax
import jax.numpy as jnp
from jax import lax
from jax.experimental import pallas as pl
from jax.experimental.pallas import tpu as pltpu
from jax.sharding import PartitionSpec as P


UNROLL = 4
VMEM_LIMIT = 8 * 1024 * 1024

in_vmem = functools.partial(pltpu.with_memory_space_constraint, memory_space=pltpu.VMEM)
in_hbm = functools.partial(pltpu.with_memory_space_constraint, memory_space=pltpu.HBM)


def mask_kernel(half_ref, acts_ref, live_ref, out_ref):
    blocks, _, block = out_ref.shape
    live = live_ref[...].astype(jnp.float32).T
    for i in range(blocks):
        x = acts_ref[:, i * block:(i + 1) * block].astype(jnp.float32)
        out_ref[i] = (x * live[:, i:i + 1]).astype(jnp.bfloat16)


def masked(acts, act_mask, first, blocks, steps=1):
    rows, width = acts.shape
    block = width // act_mask.shape[1]
    unit = blocks // steps
    return pl.pallas_call(
        mask_kernel,
        out_shape=pltpu.VMEM((blocks, rows, block), jnp.bfloat16),
        grid_spec=pltpu.PrefetchScalarGridSpec(
            num_scalar_prefetch=1,
            grid=(steps,),
            in_specs=[
                pl.BlockSpec((rows, unit * block), lambda s, f: (0, f[0] + s)),
                pl.BlockSpec((unit, rows), lambda s, f: (f[0] + s, 0)),
            ],
            out_specs=pl.BlockSpec((unit, rows, block), lambda s, f: (s, 0, 0)),
        ),
        compiler_params=pltpu.CompilerParams(vmem_limit_bytes=VMEM_LIMIT),
        cost_estimate=pl.CostEstimate(flops=rows * blocks, bytes_accessed=4 * rows * blocks * block, transcendentals=0),
    )(first.reshape(1), in_hbm(acts), in_hbm(act_mask.T))


def clear(acc):

    def body(i, carry):
        acc[i] = jnp.zeros_like(acc[i])
        return carry

    lax.fori_loop(0, acc.shape[0], body, 0, unroll=4)


def add_products(acc, x_ref, w_ref, place_ref, start, first, count):
    _, entries, block, _ = w_ref.shape

    def advance(step, carry):
        for i in range(UNROLL):
            at = first + step * UNROLL + i
            row = start + at
            x = x_ref[at]
            for k in range(0, entries, 2):
                pair = jnp.concatenate([w_ref[row, k], w_ref[row, k + 1]], axis=1)
                product = jnp.dot(x, pair, preferred_element_type=jnp.float32)
                for half in range(2):
                    to = place_ref[row * entries + k + half]
                    acc[to] = acc[to] + product[:, half * block:(half + 1) * block]
        return carry

    lax.fori_loop(0, count // UNROLL, advance, 0)


def write_out(acc, outs):
    start = 0
    for out in outs:

        def body(i, carry, out=out, start=start):
            out[i] = acc[start + i].astype(out.dtype)
            return carry

        lax.fori_loop(0, out.shape[0], body, 0, unroll=4)
        start += out.shape[0]


def fold_kernel(parts, load, starts_ref, place_ref, *refs):
    x_refs, w_ref, refs = refs[:parts], refs[parts], refs[parts + 1:]
    copies = []
    if load:
        *outs, held_ref, acc, sems = refs
        for part, x_ref in enumerate(x_refs):
            for first in range(0, x_ref.shape[0], UNROLL):
                rows = pl.ds(starts_ref[part] + first, UNROLL)
                copies.append(pltpu.make_async_copy(w_ref.at[rows], held_ref.at[rows], sems.at[len(copies)]))
        w_ref = held_ref
    else:
        *outs, acc = refs
    for copy in copies:
        copy.start()
    clear(acc)
    for part, x_ref in enumerate(x_refs):
        if load:
            for first in range(0, x_ref.shape[0], UNROLL):
                copies.pop(0).wait()
                add_products(acc, x_ref, w_ref, place_ref, starts_ref[part], first, UNROLL)
        else:
            add_products(acc, x_ref, w_ref, place_ref, starts_ref[part], 0, x_ref.shape[0])
    write_out(acc, outs)


def fold(xs, weights, places, starts, segments, load=False, keep=False):
    rows_in, entries, block, _ = weights.shape
    rows = xs[0].shape[1]
    total = sum(count for count, _ in segments)
    smem = pl.BlockSpec(memory_space=pltpu.SMEM)
    vmem = pl.BlockSpec(memory_space=pltpu.VMEM)
    hbm = pl.BlockSpec(memory_space=pltpu.HBM)
    out_shape = [pltpu.VMEM((count, rows, block), kind) for count, kind in segments]
    scratch = [pltpu.VMEM((total, rows, block), jnp.float32)]
    held = pltpu.VMEM(weights.shape, weights.dtype)
    limit = VMEM_LIMIT
    if load:
        scratch.append(pltpu.SemaphoreType.DMA((rows_in // UNROLL,)))
        if keep:
            out_shape.append(held)
        else:
            scratch.insert(0, held)
            limit += weights.size * weights.dtype.itemsize
    return pl.pallas_call(
        functools.partial(fold_kernel, len(xs), load),
        out_shape=out_shape,
        in_specs=[smem, smem] + [vmem] * len(xs) + [hbm if load else vmem],
        out_specs=[vmem] * len(out_shape),
        scratch_shapes=scratch,
        compiler_params=pltpu.CompilerParams(vmem_limit_bytes=limit),
        cost_estimate=pl.CostEstimate(
            flops=2 * rows * rows_in * entries * block * block,
            bytes_accessed=2 * weights.size,
            transcendentals=0,
        ),
    )(jnp.stack(starts), places.reshape(-1), *map(in_vmem, xs), (in_hbm if load else in_vmem)(weights))


def add_kernel(*refs):
    *parts, out_ref = refs

    def body(i, carry):
        total = parts[0][i]
        for part in parts[1:]:
            total = total + part[i].astype(jnp.float32)
        out_ref[i] = total.astype(jnp.bfloat16)
        return carry

    lax.fori_loop(0, out_ref.shape[0], body, 0, unroll=2)


def add(parts):
    vmem = pl.BlockSpec(memory_space=pltpu.VMEM)
    return pl.pallas_call(
        add_kernel,
        out_shape=pltpu.VMEM(parts[0].shape, jnp.bfloat16),
        in_specs=[vmem] * len(parts),
        out_specs=vmem,
        compiler_params=pltpu.CompilerParams(vmem_limit_bytes=VMEM_LIMIT),
    )(*map(in_vmem, parts))


def finish_kernel(mine_ref, got_ref, near_ref, *refs):
    cross_refs, bias_ref, out_ref = refs[:-2], refs[-2], refs[-1]
    share, _, block = mine_ref.shape
    size = cross_refs[0].shape[0]
    for i in range(share):
        total = mine_ref[i] + got_ref[i].astype(jnp.float32) + near_ref[i].astype(jnp.float32)
        for cross_ref in cross_refs[i // size::share // size]:
            total = total + cross_ref[i % size].astype(jnp.float32)
        total = jnp.maximum(total + bias_ref[i:i + 1, :], 0.0)
        out_ref[:, i * block:(i + 1) * block] = total.astype(jnp.bfloat16)


def exchange_plan(acts, act_mask, w1, cols1, bias1, mask2, w2, cols2, bias2):
    bf16, f32 = jnp.bfloat16, jnp.float32
    block = w1.shape[-1]
    rows = acts.shape[0]
    row_blocks = act_mask.shape[1]
    col_blocks = mask2.shape[1]
    half_in = row_blocks // 2
    half_mid = col_blocks // 2
    quarter = col_blocks // 4
    size_row, size_col = lax.axis_size("row"), lax.axis_size("col")
    r, c, d = lax.axis_index("row"), lax.axis_index("col"), lax.axis_index("depth")
    core = lax.rem(r, 2)
    over_depth = functools.partial(lax.ppermute, axis_name="depth", perm=[(0, 1), (1, 0)])
    over_core = functools.partial(lax.ppermute, axis_name="row", perm=[(i, i ^ 1) for i in range(size_row)])
    over_x = functools.partial(lax.ppermute, axis_name="row", perm=[(i, i ^ 2) for i in range(size_row)])
    zero = jnp.int32(0)

    side = lax.rem(c, 2)
    eighth, fourth = half_in // 4, half_in // 2
    part_x = over_depth(masked(acts, act_mask, (1 - d) * 4 + side, eighth))
    rest_x = over_depth(masked(acts, act_mask, (1 - d) * 2 + 1, fourth))
    own_x = masked(acts, act_mask, d * 2, half_in, steps=2)
    swapped_x = lax.ppermute(part_x, "col", [(i, i ^ 1) for i in range(size_col)])
    other_x = [part_x, swapped_x, rest_x]
    other_starts = [side * eighth, (1 - side) * eighth, jnp.int32(fourth)]
    mask_own = lax.dynamic_slice_in_dim(mask2, d * half_mid + core * quarter, quarter, 1).astype(bf16)
    mask_other = over_depth(
        lax.dynamic_slice_in_dim(mask2, (1 - d) * half_mid + core * quarter, quarter, 1).astype(bf16)
    )
    bias_blocks = lax.dynamic_slice_in_dim(
        bias1.reshape(col_blocks, 1, block), d * half_mid + core * quarter, quarter, 0
    )

    to1 = lax.dynamic_slice_in_dim(cols1, d * half_in, half_in, 0) - c * col_blocks
    to_depth = to1 // half_mid
    to_core = (to1 // quarter) % 2
    same_core = 1 - (to_core ^ core)
    same_depth = 1 - (to_depth ^ d)
    place1 = same_core * half_mid + same_depth * quarter + to1 % quarter

    to2 = lax.dynamic_slice_in_dim(cols2, d * half_mid, half_mid, 0) - r * row_blocks
    share = row_blocks // size_col
    chunk = to2 // share
    far = jnp.where(c < size_col // 2, size_col - 1, 0)
    slot = jnp.where(chunk == far, 0, jnp.where(chunk == (far ^ 1), 1, jnp.where(chunk == (c ^ 1), 2, 3)))
    place2 = slot * share + to2 % share
    own_x, place1, place2 = lax.optimization_barrier((own_x, place1, place2))

    segments = [(half_mid, bf16), (quarter, f32), (quarter, f32)]

    def core_sums(low, send, keep):
        low = over_core(low)
        return lax.optimization_barrier(
            ((send + low[:quarter].astype(f32)).astype(bf16), keep + low[quarter:].astype(f32))
        )

    sums = fold([own_x], w1, place1, [zero], segments, load=True)
    send_own, keep_own = core_sums(*sums)
    got_other = over_depth(send_own)
    sums = fold(other_x, w1, place1, other_starts, segments, load=True)
    send_other, keep_other = core_sums(*sums)
    got_own = over_depth(send_other)

    def x_sums(keep, got):
        part = keep + got.astype(f32)
        part, low = lax.optimization_barrier((part, part.astype(bf16)))
        return part, over_x(low)

    def hidden(part, low, mask):
        z1 = part + low.astype(f32)
        out = (jnp.maximum(z1 + bias_blocks, 0.0) * mask.astype(f32).T[:, :, None]).astype(bf16)
        out = lax.optimization_barrier(out)
        return [out, over_core(out)]

    sums_other = x_sums(keep_other, got_other)
    sums_own = x_sums(keep_own, got_own)
    hidden_other = hidden(*sums_other, mask_other)
    starts = [core * quarter, (1 - core) * quarter]
    cuts = [share // 2] * 4 + [share] * 2
    *for_other, w2 = fold(hidden_other, w2, place2, starts, [(n, bf16) for n in cuts], load=True, keep=True)
    got = []
    for part in for_other:
        got.append(over_depth(part))
    part_own, low_own, w2 = lax.optimization_barrier((*sums_own, w2))
    hidden_own = hidden(part_own, low_own, mask_own)
    mine = fold(hidden_own, w2, place2, starts, [(n, f32) for n in cuts])

    def over_col(parts, perm):
        return lax.ppermute(add(parts), "col", perm)

    cross = []
    for i in range(4):
        total = [mine[i], got[i]]
        total.append(over_col(total, [(0, 1), (3, 2)]))
        cross.append(over_col(total, [(1, 3), (2, 0)] if i < 2 else [(1, 2), (2, 1)]))
    near = over_col([mine[4], got[4]], [(i, i ^ 1) for i in range(size_col)])
    parts = [mine[5], got[5], near, *cross]
    return pl.pallas_call(
        finish_kernel,
        out_shape=jax.ShapeDtypeStruct((rows, share * block), bf16),
        compiler_params=pltpu.CompilerParams(vmem_limit_bytes=VMEM_LIMIT),
    )(*map(in_vmem, parts), bias2.reshape(share, block))


def fold_function(inputs, targets, stride):

    def add_tiles(running_total, tiles):

        def advance(number, total):
            offset = number * stride
            block_list = lax.dynamic_slice_in_dim(tiles, offset, stride, 0)
            incoming_rows = lax.dynamic_slice_in_dim(inputs, offset, stride, 1)
            wanted = lax.dynamic_slice_in_dim(targets, offset, stride, 0)
            product = jnp.einsum(
                "tws,wish->twih", incoming_rows, block_list, preferred_element_type=jnp.float32
            )
            flat_product = product.reshape(product.shape[0], -1, product.shape[-1])
            return total.at[:, wanted.reshape(-1)].add(flat_product)

        return lax.fori_loop(0, tiles.shape[0] // stride, advance, running_total)

    return add_tiles


def gather_plan(acts, act_mask, w1, cols1, bias1, mask2, w2, cols2, bias2):
    block = w1.shape[-1]
    rows_dev = acts.shape[0]
    row_blocks = act_mask.shape[1]
    col_blocks = mask2.shape[1]
    row_index = lax.axis_index("row")
    col_index = lax.axis_index("col")
    masked = acts.reshape(rows_dev, row_blocks, block) * act_mask[:, :, None].astype(jnp.bfloat16)
    first_targets = cols1 - col_index * col_blocks
    second_targets = cols2 - row_index * row_blocks
    first_fold = fold_function(masked, first_targets, w1.shape[0])
    first_sum = first_fold(
        jnp.zeros((rows_dev, col_blocks, block), jnp.float32), lax.all_gather(w1, "depth", axis=0, tiled=True)
    )
    bias_blocks = bias1.reshape(col_blocks, block)
    share = col_blocks // lax.axis_size("row")
    part_sum = lax.psum_scatter(first_sum, "row", scatter_dimension=1, tiled=True)
    bias_part = lax.dynamic_slice_in_dim(bias_blocks, row_index * share, share, 0)
    mask_part = lax.dynamic_slice_in_dim(mask2, row_index * share, share, 1)
    hidden_part = jnp.maximum(part_sum + bias_part, 0.0) * mask_part[:, :, None].astype(jnp.float32)
    hidden = lax.all_gather(hidden_part.astype(jnp.bfloat16), "row", axis=1, tiled=True)
    second_fold = fold_function(hidden, second_targets, w2.shape[0])
    second_sum = second_fold(
        jnp.zeros((rows_dev, row_blocks, block), jnp.float32), lax.all_gather(w2, "depth", axis=0, tiled=True)
    )
    outcome = lax.psum_scatter(second_sum, "col", scatter_dimension=1, tiled=True)
    bias_out = bias2.reshape(outcome.shape[1], block)
    return jnp.maximum(outcome + bias_out, 0.0).astype(jnp.bfloat16).reshape(rows_dev, -1)


def solution(mesh):
    sizes = dict(mesh.shape)
    pairs = sizes["depth"] == 2 and sizes["row"] == 4 and sizes["col"] == 4
    return jax.shard_map(
        exchange_plan if pairs else gather_plan,
        mesh=mesh,
        in_specs=(
            P("depth", "row"),
            P("depth", "row"),
            P(("row", "depth"), "col", None, None),
            P("row", "col"),
            P("col"),
            P("depth", "col"),
            P(("col", "depth"), "row", None, None),
            P("col", "row"),
            P(("row", "col")),
        ),
        out_specs=P("depth", ("row", "col")),
        check_vma=False,
    )
```

```python
import functools

import jax
import jax.numpy as jnp
from jax import lax
from jax.experimental import pallas as pl
from jax.experimental.pallas import tpu as pltpu
from jax.sharding import PartitionSpec as P


UNROLL = 4
GROUPS = 4
VMEM_LIMIT = 8 * 1024 * 1024

in_vmem = functools.partial(pltpu.with_memory_space_constraint, memory_space=pltpu.VMEM)
in_hbm = functools.partial(pltpu.with_memory_space_constraint, memory_space=pltpu.HBM)


def mask_kernel(half_ref, acts_ref, live_ref, out_ref):
    blocks, _, block = out_ref.shape
    live = live_ref[...].astype(jnp.float32).T
    for i in range(blocks):
        x = acts_ref[:, i * block:(i + 1) * block].astype(jnp.float32)
        out_ref[i] = (x * live[:, i:i + 1]).astype(jnp.bfloat16)


def masked(acts, act_mask, first, blocks, steps=1):
    rows, width = acts.shape
    block = width // act_mask.shape[1]
    unit = blocks // steps
    return pl.pallas_call(
        mask_kernel,
        out_shape=pltpu.VMEM((blocks, rows, block), jnp.bfloat16),
        grid_spec=pltpu.PrefetchScalarGridSpec(
            num_scalar_prefetch=1,
            grid=(steps,),
            in_specs=[
                pl.BlockSpec((rows, unit * block), lambda s, f: (0, f[0] + s)),
                pl.BlockSpec((unit, rows), lambda s, f: (f[0] + s, 0)),
            ],
            out_specs=pl.BlockSpec((unit, rows, block), lambda s, f: (s, 0, 0)),
        ),
        compiler_params=pltpu.CompilerParams(vmem_limit_bytes=VMEM_LIMIT),
        cost_estimate=pl.CostEstimate(flops=rows * blocks, bytes_accessed=4 * rows * blocks * block, transcendentals=0),
    )(first.reshape(1), in_hbm(acts), in_hbm(act_mask.T))


def clear(acc):

    def body(i, carry):
        acc[i] = jnp.zeros_like(acc[i])
        return carry

    lax.fori_loop(0, acc.shape[0], body, 0, unroll=4)


def add_row(acc, x, w_ref, tables, row):
    scalars, cols_ref = tables
    _, entries, block, _ = w_ref.shape
    group = acc.shape[0] // GROUPS
    for k in range(0, entries, 2):
        pair = jnp.concatenate([w_ref[row, k], w_ref[row, k + 1]], axis=1)
        product = jnp.dot(x, pair, preferred_element_type=jnp.float32)
        for half in range(2):
            col = cols_ref[k + half, scalars[0] + row] - scalars[1]
            which = sum((col >= i * group).astype(jnp.int32) for i in range(1, GROUPS))
            to = col + scalars[2 + which]
            acc[to] = acc[to] + product[:, half * block:(half + 1) * block]


def add_products(acc, x_ref, w_ref, tables, start, first, count):
    def advance(step, carry):
        for i in range(UNROLL):
            at = first + step * UNROLL + i
            add_row(acc, x_ref[at], w_ref, tables, start + at)
        return carry

    lax.fori_loop(0, count // UNROLL, advance, 0)


def write_out(acc, outs):
    start = 0
    for out in outs:

        def body(i, carry, out=out, start=start):
            out[i] = acc[start + i].astype(out.dtype)
            return carry

        lax.fori_loop(0, out.shape[0], body, 0, unroll=4)
        start += out.shape[0]


def row_copies(w_ref, held_ref, sems, ranges):
    copies = []
    for start, count in ranges:
        for first in range(0, count, UNROLL):
            rows = pl.ds(start + first, UNROLL)
            copies.append(pltpu.make_async_copy(w_ref.at[rows], held_ref.at[rows], sems.at[len(copies)]))
    return copies


def fold_kernel(parts, load, scalars, cols_ref, *refs):
    x_refs, w_ref, refs = refs[:parts], refs[parts], refs[parts + 1:]
    tables = scalars, cols_ref
    starts = [scalars[2 + GROUPS + i] for i in range(parts)]
    copies = []
    if load:
        *outs, held_ref, acc, sems = refs
        copies = row_copies(w_ref, held_ref, sems, [(at, x.shape[0]) for at, x in zip(starts, x_refs)])
        w_ref = held_ref
    else:
        *outs, acc = refs
    for copy in copies:
        copy.start()
    clear(acc)
    for start, x_ref in zip(starts, x_refs):
        if load:
            for first in range(0, x_ref.shape[0], UNROLL):
                copies.pop(0).wait()
                add_products(acc, x_ref, w_ref, tables, start, first, UNROLL)
        else:
            add_products(acc, x_ref, w_ref, tables, start, 0, x_ref.shape[0])
    write_out(acc, outs)


def own_fold_kernel(scalars, cols_ref, acts_ref, live_ref, w_ref, *refs):
    *outs, held_ref, acc, x_ref, mask_ref, sems = refs
    blocks = w_ref.shape[0]
    width = x_ref.shape[1]
    block = width // blocks
    count = blocks // UNROLL
    half = scalars[2 + GROUPS]
    lanes = pl.ds(pl.multiple_of(half * width, width), width)
    inputs = [
        pltpu.make_async_copy(live_ref.at[pl.ds(half * blocks, blocks)], mask_ref, sems.at[count]),
        pltpu.make_async_copy(acts_ref.at[:, lanes], x_ref, sems.at[count + 1]),
    ]
    copies = row_copies(w_ref, held_ref, sems, [(0, blocks)])
    for copy in inputs + copies:
        copy.start()
    clear(acc)
    for copy in inputs:
        copy.wait()
    live = mask_ref[...].astype(jnp.float32).T
    for i, copy in enumerate(copies):
        copy.wait()
        for at in range(i * UNROLL, (i + 1) * UNROLL):
            x = x_ref[:, at * block:(at + 1) * block].astype(jnp.float32) * live[:, at:at + 1]
            add_row(acc, x.astype(jnp.bfloat16), held_ref, (scalars, cols_ref), at)
    write_out(acc, outs)


def fold_parts(rows, weights, segments):
    block = weights.shape[-1]
    outs = [pltpu.VMEM((count, rows, block), kind) for count, kind in segments]
    acc = pltpu.VMEM((sum(count for count, _ in segments), rows, block), jnp.float32)
    held = pltpu.VMEM(weights.shape, weights.dtype)
    cost = pl.CostEstimate(flops=2 * rows * weights.size, bytes_accessed=2 * weights.size, transcendentals=0)
    return outs, acc, held, weights.shape[0] // UNROLL, cost


def own_fold(acts, act_mask, half, weights, cols, scalars, segments):
    rows, width = acts.shape
    outs, acc, held, count, cost = fold_parts(rows, weights, segments)
    smem = pl.BlockSpec(memory_space=pltpu.SMEM)
    vmem = pl.BlockSpec(memory_space=pltpu.VMEM)
    hbm = pl.BlockSpec(memory_space=pltpu.HBM)
    return pl.pallas_call(
        own_fold_kernel,
        out_shape=outs,
        in_specs=[smem, smem, hbm, hbm, hbm],
        out_specs=[vmem] * len(outs),
        scratch_shapes=[
            held,
            acc,
            pltpu.VMEM((rows, width // 2), acts.dtype),
            pltpu.VMEM((weights.shape[0], rows), act_mask.dtype),
            pltpu.SemaphoreType.DMA((count + 2,)),
        ],
        compiler_params=pltpu.CompilerParams(vmem_limit_bytes=2 * VMEM_LIMIT + 2 * 1024 * 1024),
        cost_estimate=cost,
    )(jnp.stack([*scalars, half]), cols.T, in_hbm(acts), in_hbm(act_mask.T), in_hbm(weights))


def fold(xs, weights, cols, scalars, starts, segments, load=False, keep=False):
    outs, acc, held, count, cost = fold_parts(xs[0].shape[1], weights, segments)
    scratch = [acc]
    smem = pl.BlockSpec(memory_space=pltpu.SMEM)
    vmem = pl.BlockSpec(memory_space=pltpu.VMEM)
    hbm = pl.BlockSpec(memory_space=pltpu.HBM)
    limit = VMEM_LIMIT
    if load:
        scratch.append(pltpu.SemaphoreType.DMA((count,)))
        if keep:
            outs.append(held)
        else:
            scratch.insert(0, held)
            limit += weights.size * weights.dtype.itemsize
    return pl.pallas_call(
        functools.partial(fold_kernel, len(xs), load),
        out_shape=outs,
        in_specs=[smem, smem] + [vmem] * len(xs) + [hbm if load else vmem],
        out_specs=[vmem] * len(outs),
        scratch_shapes=scratch,
        compiler_params=pltpu.CompilerParams(vmem_limit_bytes=limit),
        cost_estimate=cost,
    )(jnp.stack([*scalars, *starts]), cols.T, *map(in_vmem, xs), (in_hbm if load else in_vmem)(weights))


def add_kernel(*refs):
    *parts, out_ref = refs

    def body(i, carry):
        total = parts[0][i]
        for part in parts[1:]:
            total = total + part[i].astype(jnp.float32)
        out_ref[i] = total.astype(jnp.bfloat16)
        return carry

    lax.fori_loop(0, out_ref.shape[0], body, 0, unroll=2)


def add(parts):
    vmem = pl.BlockSpec(memory_space=pltpu.VMEM)
    return pl.pallas_call(
        add_kernel,
        out_shape=pltpu.VMEM(parts[0].shape, jnp.bfloat16),
        in_specs=[vmem] * len(parts),
        out_specs=vmem,
        compiler_params=pltpu.CompilerParams(vmem_limit_bytes=VMEM_LIMIT),
    )(*map(in_vmem, parts))


def finish_kernel(mine_ref, got_ref, near_ref, *refs):
    cross_refs, bias_ref, out_ref = refs[:-2], refs[-2], refs[-1]
    share, _, block = mine_ref.shape
    size = cross_refs[0].shape[0]
    for i in range(share):
        total = mine_ref[i] + got_ref[i].astype(jnp.float32) + near_ref[i].astype(jnp.float32)
        for cross_ref in cross_refs[i // size::share // size]:
            total = total + cross_ref[i % size].astype(jnp.float32)
        total = jnp.maximum(total + bias_ref[i:i + 1, :], 0.0)
        out_ref[:, i * block:(i + 1) * block] = total.astype(jnp.bfloat16)


def exchange_plan(acts, act_mask, w1, cols1, bias1, mask2, w2, cols2, bias2):
    bf16, f32 = jnp.bfloat16, jnp.float32
    block = w1.shape[-1]
    rows = acts.shape[0]
    row_blocks = act_mask.shape[1]
    col_blocks = mask2.shape[1]
    half_in = row_blocks // 2
    half_mid = col_blocks // 2
    quarter = col_blocks // 4
    size_row, size_col = lax.axis_size("row"), lax.axis_size("col")
    r, c, d = lax.axis_index("row"), lax.axis_index("col"), lax.axis_index("depth")
    core = lax.rem(r, 2)
    over_depth = functools.partial(lax.ppermute, axis_name="depth", perm=[(0, 1), (1, 0)])
    over_core = functools.partial(lax.ppermute, axis_name="row", perm=[(i, i ^ 1) for i in range(size_row)])
    over_x = functools.partial(lax.ppermute, axis_name="row", perm=[(i, i ^ 2) for i in range(size_row)])

    side = lax.rem(c, 2)
    eighth, fourth = half_in // 4, half_in // 2
    part_x = over_depth(masked(acts, act_mask, (1 - d) * 4 + side, eighth))
    rest_x = over_depth(masked(acts, act_mask, (1 - d) * 2 + 1, fourth))
    swapped_x = lax.ppermute(part_x, "col", [(i, i ^ 1) for i in range(size_col)])
    other_x = [part_x, swapped_x, rest_x]
    other_starts = [side * eighth, (1 - side) * eighth, jnp.int32(fourth)]
    mask_own = lax.dynamic_slice_in_dim(mask2, d * half_mid + core * quarter, quarter, 1).astype(bf16)
    mask_other = over_depth(
        lax.dynamic_slice_in_dim(mask2, (1 - d) * half_mid + core * quarter, quarter, 1).astype(bf16)
    )
    bias_blocks = lax.dynamic_slice_in_dim(
        bias1.reshape(col_blocks, 1, block), d * half_mid + core * quarter, quarter, 0
    )

    def shifts(places, size):
        return [(place - i) * size for i, place in enumerate(places)]

    places1 = [(1 - (which ^ core)) * 2 + 1 - (depth ^ d) for depth in range(2) for which in range(2)]
    scalars1 = [d * half_in, c * col_blocks, *shifts(places1, quarter)]

    share = row_blocks // size_col
    far = jnp.where(c < size_col // 2, size_col - 1, 0)
    places2 = [
        jnp.where(i == far, 0, jnp.where(i == (far ^ 1), 1, jnp.where(i == (c ^ 1), 2, 3))) for i in range(size_col)
    ]
    scalars2 = [d * half_mid, r * row_blocks, *shifts(places2, share)]
    segments = [(half_mid, bf16), (quarter, f32), (quarter, f32)]

    def core_sums(low, send, keep):
        low = over_core(low)
        return lax.optimization_barrier(
            ((send + low[:quarter].astype(f32)).astype(bf16), keep + low[quarter:].astype(f32))
        )

    sums = own_fold(acts, act_mask, d, w1, cols1, scalars1, segments)
    send_own, keep_own = core_sums(*sums)
    got_other = over_depth(send_own)
    sums = fold(other_x, w1, cols1, scalars1, other_starts, segments, load=True)
    send_other, keep_other = core_sums(*sums)
    got_own = over_depth(send_other)

    def x_sums(keep, got):
        part = keep + got.astype(f32)
        part, low = lax.optimization_barrier((part, part.astype(bf16)))
        return part, over_x(low)

    def hidden(part, low, mask):
        z1 = part + low.astype(f32)
        out = (jnp.maximum(z1 + bias_blocks, 0.0) * mask.astype(f32).T[:, :, None]).astype(bf16)
        out = lax.optimization_barrier(out)
        return [out, over_core(out)]

    sums_other = x_sums(keep_other, got_other)
    sums_own = x_sums(keep_own, got_own)
    hidden_other = hidden(*sums_other, mask_other)
    starts = [core * quarter, (1 - core) * quarter]
    cuts = [share // 2] * 4 + [share] * 2
    *for_other, w2 = fold(hidden_other, w2, cols2, scalars2, starts, [(n, bf16) for n in cuts], load=True, keep=True)
    got = []
    for part in for_other:
        got.append(over_depth(part))
    part_own, low_own, w2 = lax.optimization_barrier((*sums_own, w2))
    hidden_own = hidden(part_own, low_own, mask_own)
    mine = fold(hidden_own, w2, cols2, scalars2, starts, [(n, f32) for n in cuts])

    def over_col(parts, perm):
        return lax.ppermute(add(parts), "col", perm)

    cross = []
    for i in range(4):
        total = [mine[i], got[i]]
        total.append(over_col(total, [(0, 1), (3, 2)]))
        cross.append(over_col(total, [(1, 3), (2, 0)] if i < 2 else [(1, 2), (2, 1)]))
    near = over_col([mine[4], got[4]], [(i, i ^ 1) for i in range(size_col)])
    parts = [mine[5], got[5], near, *cross]
    return pl.pallas_call(
        finish_kernel,
        out_shape=jax.ShapeDtypeStruct((rows, share * block), bf16),
        compiler_params=pltpu.CompilerParams(vmem_limit_bytes=VMEM_LIMIT),
    )(*map(in_vmem, parts), bias2.reshape(share, block))


def fold_function(inputs, targets, stride):

    def add_tiles(running_total, tiles):

        def advance(number, total):
            offset = number * stride
            block_list = lax.dynamic_slice_in_dim(tiles, offset, stride, 0)
            incoming_rows = lax.dynamic_slice_in_dim(inputs, offset, stride, 1)
            wanted = lax.dynamic_slice_in_dim(targets, offset, stride, 0)
            product = jnp.einsum(
                "tws,wish->twih", incoming_rows, block_list, preferred_element_type=jnp.float32
            )
            flat_product = product.reshape(product.shape[0], -1, product.shape[-1])
            return total.at[:, wanted.reshape(-1)].add(flat_product)

        return lax.fori_loop(0, tiles.shape[0] // stride, advance, running_total)

    return add_tiles


def gather_plan(acts, act_mask, w1, cols1, bias1, mask2, w2, cols2, bias2):
    block = w1.shape[-1]
    rows_dev = acts.shape[0]
    row_blocks = act_mask.shape[1]
    col_blocks = mask2.shape[1]
    row_index = lax.axis_index("row")
    col_index = lax.axis_index("col")
    masked = acts.reshape(rows_dev, row_blocks, block) * act_mask[:, :, None].astype(jnp.bfloat16)
    first_targets = cols1 - col_index * col_blocks
    second_targets = cols2 - row_index * row_blocks
    first_fold = fold_function(masked, first_targets, w1.shape[0])
    first_sum = first_fold(
        jnp.zeros((rows_dev, col_blocks, block), jnp.float32), lax.all_gather(w1, "depth", axis=0, tiled=True)
    )
    bias_blocks = bias1.reshape(col_blocks, block)
    share = col_blocks // lax.axis_size("row")
    part_sum = lax.psum_scatter(first_sum, "row", scatter_dimension=1, tiled=True)
    bias_part = lax.dynamic_slice_in_dim(bias_blocks, row_index * share, share, 0)
    mask_part = lax.dynamic_slice_in_dim(mask2, row_index * share, share, 1)
    hidden_part = jnp.maximum(part_sum + bias_part, 0.0) * mask_part[:, :, None].astype(jnp.float32)
    hidden = lax.all_gather(hidden_part.astype(jnp.bfloat16), "row", axis=1, tiled=True)
    second_fold = fold_function(hidden, second_targets, w2.shape[0])
    second_sum = second_fold(
        jnp.zeros((rows_dev, row_blocks, block), jnp.float32), lax.all_gather(w2, "depth", axis=0, tiled=True)
    )
    outcome = lax.psum_scatter(second_sum, "col", scatter_dimension=1, tiled=True)
    bias_out = bias2.reshape(outcome.shape[1], block)
    return jnp.maximum(outcome + bias_out, 0.0).astype(jnp.bfloat16).reshape(rows_dev, -1)


def solution(mesh):
    sizes = dict(mesh.shape)
    pairs = sizes["depth"] == 2 and sizes["row"] == 4 and sizes["col"] == 4
    return jax.shard_map(
        exchange_plan if pairs else gather_plan,
        mesh=mesh,
        in_specs=(
            P("depth", "row"),
            P("depth", "row"),
            P(("row", "depth"), "col", None, None),
            P("row", "col"),
            P("col"),
            P("depth", "col"),
            P(("col", "depth"), "row", None, None),
            P("col", "row"),
            P(("row", "col")),
        ),
        out_specs=P("depth", ("row", "col")),
        check_vma=False,
    )
```

```python
import functools

import jax
import jax.numpy as jnp
from jax import lax
from jax.experimental import pallas as pl
from jax.experimental.pallas import tpu as pltpu
from jax.sharding import PartitionSpec as P


UNROLL = 4
GROUPS = 4
VMEM_LIMIT = 8 * 1024 * 1024

in_vmem = functools.partial(pltpu.with_memory_space_constraint, memory_space=pltpu.VMEM)
in_hbm = functools.partial(pltpu.with_memory_space_constraint, memory_space=pltpu.HBM)


def mask_kernel(half_ref, acts_ref, live_ref, out_ref):
    blocks, _, block = out_ref.shape
    live = live_ref[...].astype(jnp.float32).T
    for i in range(blocks):
        x = acts_ref[:, i * block:(i + 1) * block].astype(jnp.float32)
        out_ref[i] = (x * live[:, i:i + 1]).astype(jnp.bfloat16)


def masked(acts, act_mask, first, blocks, steps=1):
    rows, width = acts.shape
    block = width // act_mask.shape[1]
    unit = blocks // steps
    return pl.pallas_call(
        mask_kernel,
        out_shape=pltpu.VMEM((blocks, rows, block), jnp.bfloat16),
        grid_spec=pltpu.PrefetchScalarGridSpec(
            num_scalar_prefetch=1,
            grid=(steps,),
            in_specs=[
                pl.BlockSpec((rows, unit * block), lambda s, f: (0, f[0] + s)),
                pl.BlockSpec((unit, rows), lambda s, f: (f[0] + s, 0)),
            ],
            out_specs=pl.BlockSpec((unit, rows, block), lambda s, f: (s, 0, 0)),
        ),
        compiler_params=pltpu.CompilerParams(vmem_limit_bytes=VMEM_LIMIT),
        cost_estimate=pl.CostEstimate(flops=rows * blocks, bytes_accessed=4 * rows * blocks * block, transcendentals=0),
    )(first.reshape(1), in_hbm(acts), in_hbm(act_mask.T))


def clear(acc):

    def body(i, carry):
        acc[i] = jnp.zeros_like(acc[i])
        return carry

    lax.fori_loop(0, acc.shape[0], body, 0, unroll=4)


def add_row(acc, x, w_ref, tables, row):
    scalars, cols_ref = tables
    _, entries, block, _ = w_ref.shape
    group = acc.shape[0] // GROUPS
    for k in range(0, entries, 2):
        pair = jnp.concatenate([w_ref[row, k], w_ref[row, k + 1]], axis=1)
        product = jnp.dot(x, pair, preferred_element_type=jnp.float32)
        for half in range(2):
            col = cols_ref[k + half, scalars[0] + row]
            if group & (group - 1):
                which = lax.rem(lax.div(col, group), GROUPS)
            else:
                which = (col >> (group.bit_length() - 1)) & (GROUPS - 1)
            to = col + scalars[1 + which]
            acc[to] = acc[to] + product[:, half * block:(half + 1) * block]


def add_products(acc, x_ref, w_ref, tables, start, first, count):
    unroll = 2 * UNROLL if count % (2 * UNROLL) == 0 else UNROLL

    def advance(step, carry):
        for i in range(unroll):
            at = first + step * unroll + i
            add_row(acc, x_ref[at], w_ref, tables, start + at)
        return carry

    lax.fori_loop(0, count // unroll, advance, 0)


def write_out(acc, outs):
    start = 0
    for out in outs:

        def body(i, carry, out=out, start=start):
            out[i] = acc[start + i].astype(out.dtype)
            return carry

        lax.fori_loop(0, out.shape[0], body, 0, unroll=4)
        start += out.shape[0]


def row_copies(w_ref, held_ref, sems, ranges):
    copies = []
    sem = done = 0
    for start, count in ranges:
        pieces = []
        first = 0
        while first < count:
            size = min(count - first, max(done, UNROLL))
            rows = pl.ds(start + first, size)
            pieces.append((first, size, pltpu.make_async_copy(w_ref.at[rows], held_ref.at[rows], sems.at[sem])))
            sem, done, first = sem + 1, done + size, first + size
        copies.append(pieces)
    return copies


def fold_kernel(parts, load, scalars, cols_ref, *refs):
    x_refs, w_ref, refs = refs[:parts], refs[parts], refs[parts + 1:]
    tables = scalars, cols_ref
    starts = [scalars[1 + GROUPS + i] for i in range(parts)]
    copies = []
    if load:
        *outs, held_ref, acc, sems = refs
        copies = row_copies(w_ref, held_ref, sems, [(at, x.shape[0]) for at, x in zip(starts, x_refs)])
        w_ref = held_ref
    else:
        *outs, acc = refs
    for pieces in copies:
        for _, _, copy in pieces:
            copy.start()
    clear(acc)
    for start, x_ref in zip(starts, x_refs):
        if load:
            for first, size, copy in copies.pop(0):
                copy.wait()
                add_products(acc, x_ref, w_ref, tables, start, first, size)
        else:
            add_products(acc, x_ref, w_ref, tables, start, 0, x_ref.shape[0])
    write_out(acc, outs)


def own_fold_kernel(scalars, cols_ref, acts_ref, live_ref, w_ref, *refs):
    *outs, held_ref, acc, x_ref, mask_ref, sems = refs
    blocks = w_ref.shape[0]
    width = x_ref.shape[1]
    block = width // blocks
    count = blocks // UNROLL
    half = scalars[1 + GROUPS]
    lanes = pl.ds(pl.multiple_of(half * width, width), width)
    inputs = [
        pltpu.make_async_copy(live_ref.at[pl.ds(half * blocks, blocks)], mask_ref, sems.at[count]),
        pltpu.make_async_copy(acts_ref.at[:, lanes], x_ref, sems.at[count + 1]),
    ]
    (pieces,) = row_copies(w_ref, held_ref, sems, [(0, blocks)])
    for copy in inputs + [piece[2] for piece in pieces]:
        copy.start()
    clear(acc)
    for copy in inputs:
        copy.wait()
    live = mask_ref[...].astype(jnp.float32).T
    for first, size, copy in pieces:
        copy.wait()
        for at in range(first, first + size):
            x = x_ref[:, at * block:(at + 1) * block].astype(jnp.float32) * live[:, at:at + 1]
            add_row(acc, x.astype(jnp.bfloat16), held_ref, (scalars, cols_ref), at)
    write_out(acc, outs)


def fold_parts(rows, weights, segments):
    block = weights.shape[-1]
    outs = [pltpu.VMEM((count, rows, block), kind) for count, kind in segments]
    acc = pltpu.VMEM((sum(count for count, _ in segments), rows, block), jnp.float32)
    held = pltpu.VMEM(weights.shape, weights.dtype)
    cost = pl.CostEstimate(flops=2 * rows * weights.size, bytes_accessed=2 * weights.size, transcendentals=0)
    return outs, acc, held, weights.shape[0] // UNROLL, cost


def own_fold(acts, act_mask, half, weights, cols, scalars, segments):
    rows, width = acts.shape
    outs, acc, held, count, cost = fold_parts(rows, weights, segments)
    smem = pl.BlockSpec(memory_space=pltpu.SMEM)
    vmem = pl.BlockSpec(memory_space=pltpu.VMEM)
    hbm = pl.BlockSpec(memory_space=pltpu.HBM)
    return pl.pallas_call(
        own_fold_kernel,
        out_shape=outs,
        in_specs=[smem, smem, hbm, hbm, hbm],
        out_specs=[vmem] * len(outs),
        scratch_shapes=[
            held,
            acc,
            pltpu.VMEM((rows, width // 2), acts.dtype),
            pltpu.VMEM((weights.shape[0], rows), act_mask.dtype),
            pltpu.SemaphoreType.DMA((count + 2,)),
        ],
        compiler_params=pltpu.CompilerParams(vmem_limit_bytes=2 * VMEM_LIMIT + 2 * 1024 * 1024),
        cost_estimate=cost,
    )(jnp.stack([*scalars, half]), cols.T, in_hbm(acts), in_hbm(act_mask.T), in_hbm(weights))


def fold(xs, weights, cols, scalars, starts, segments, load=False, keep=False):
    outs, acc, held, count, cost = fold_parts(xs[0].shape[1], weights, segments)
    scratch = [acc]
    smem = pl.BlockSpec(memory_space=pltpu.SMEM)
    vmem = pl.BlockSpec(memory_space=pltpu.VMEM)
    hbm = pl.BlockSpec(memory_space=pltpu.HBM)
    limit = VMEM_LIMIT
    if load:
        scratch.append(pltpu.SemaphoreType.DMA((count,)))
        if keep:
            outs.append(held)
        else:
            scratch.insert(0, held)
            limit += weights.size * weights.dtype.itemsize
    return pl.pallas_call(
        functools.partial(fold_kernel, len(xs), load),
        out_shape=outs,
        in_specs=[smem, smem] + [vmem] * len(xs) + [hbm if load else vmem],
        out_specs=[vmem] * len(outs),
        scratch_shapes=scratch,
        compiler_params=pltpu.CompilerParams(vmem_limit_bytes=limit),
        cost_estimate=cost,
    )(jnp.stack([*scalars, *starts]), cols.T, *map(in_vmem, xs), (in_hbm if load else in_vmem)(weights))


def add_kernel(*refs):
    *parts, out_ref = refs

    def body(i, carry):
        total = parts[0][i]
        for part in parts[1:]:
            total = total + part[i].astype(jnp.float32)
        out_ref[i] = total.astype(jnp.bfloat16)
        return carry

    lax.fori_loop(0, out_ref.shape[0], body, 0, unroll=2)


def add(parts):
    vmem = pl.BlockSpec(memory_space=pltpu.VMEM)
    return pl.pallas_call(
        add_kernel,
        out_shape=pltpu.VMEM(parts[0].shape, jnp.bfloat16),
        in_specs=[vmem] * len(parts),
        out_specs=vmem,
        compiler_params=pltpu.CompilerParams(vmem_limit_bytes=VMEM_LIMIT),
    )(*map(in_vmem, parts))


def finish_kernel(mine_ref, got_ref, near_ref, *refs):
    cross_refs, bias_ref, out_ref = refs[:-2], refs[-2], refs[-1]
    share, _, block = mine_ref.shape
    size = cross_refs[0].shape[0]
    for i in range(share):
        total = mine_ref[i] + got_ref[i].astype(jnp.float32) + near_ref[i].astype(jnp.float32)
        for cross_ref in cross_refs[i // size::share // size]:
            total = total + cross_ref[i % size].astype(jnp.float32)
        total = jnp.maximum(total + bias_ref[i:i + 1, :], 0.0)
        out_ref[:, i * block:(i + 1) * block] = total.astype(jnp.bfloat16)


def exchange_plan(acts, act_mask, w1, cols1, bias1, mask2, w2, cols2, bias2):
    bf16, f32 = jnp.bfloat16, jnp.float32
    block = w1.shape[-1]
    rows = acts.shape[0]
    row_blocks = act_mask.shape[1]
    col_blocks = mask2.shape[1]
    half_in = row_blocks // 2
    half_mid = col_blocks // 2
    quarter = col_blocks // 4
    size_row, size_col = lax.axis_size("row"), lax.axis_size("col")
    r, c, d = lax.axis_index("row"), lax.axis_index("col"), lax.axis_index("depth")
    core = lax.rem(r, 2)
    over_depth = functools.partial(lax.ppermute, axis_name="depth", perm=[(0, 1), (1, 0)])
    over_core = functools.partial(lax.ppermute, axis_name="row", perm=[(i, i ^ 1) for i in range(size_row)])
    over_x = functools.partial(lax.ppermute, axis_name="row", perm=[(i, i ^ 2) for i in range(size_row)])

    side = lax.rem(c, 2)
    eighth, fourth = half_in // 4, half_in // 2
    part_x = over_depth(masked(acts, act_mask, (1 - d) * 4 + side, eighth))
    rest_x = over_depth(masked(acts, act_mask, (1 - d) * 2 + 1, fourth))
    swapped_x = lax.ppermute(part_x, "col", [(i, i ^ 1) for i in range(size_col)])
    other_x = [part_x, swapped_x, rest_x]
    other_starts = [side * eighth, (1 - side) * eighth, jnp.int32(fourth)]
    mask_own = lax.dynamic_slice_in_dim(mask2, d * half_mid + core * quarter, quarter, 1).astype(bf16)
    mask_other = over_depth(
        lax.dynamic_slice_in_dim(mask2, (1 - d) * half_mid + core * quarter, quarter, 1).astype(bf16)
    )
    bias_blocks = lax.dynamic_slice_in_dim(
        bias1.reshape(col_blocks, 1, block), d * half_mid + core * quarter, quarter, 0
    )

    def shifts(places, size, first):
        return [(place - i) * size - first for i, place in enumerate(places)]

    places1 = [(1 - (which ^ core)) * 2 + 1 - (depth ^ d) for depth in range(2) for which in range(2)]
    scalars1 = [d * half_in, *shifts(places1, quarter, c * col_blocks)]

    share = row_blocks // size_col
    far = jnp.where(c < size_col // 2, size_col - 1, 0)
    places2 = [
        jnp.where(i == far, 0, jnp.where(i == (far ^ 1), 1, jnp.where(i == (c ^ 1), 2, 3))) for i in range(size_col)
    ]
    scalars2 = [d * half_mid, *shifts(places2, share, r * row_blocks)]
    segments = [(half_mid, bf16), (quarter, f32), (quarter, f32)]

    def core_sums(low, send, keep):
        low = over_core(low)
        return lax.optimization_barrier(
            ((send + low[:quarter].astype(f32)).astype(bf16), keep + low[quarter:].astype(f32))
        )

    sums = own_fold(acts, act_mask, d, w1, cols1, scalars1, segments)
    send_own, keep_own = core_sums(*sums)
    got_other = over_depth(send_own)
    sums = fold(other_x, w1, cols1, scalars1, other_starts, segments, load=True)
    send_other, keep_other = core_sums(*sums)
    got_own = over_depth(send_other)

    def x_sums(keep, got):
        part = keep + got.astype(f32)
        part, low = lax.optimization_barrier((part, part.astype(bf16)))
        return part, over_x(low)

    def hidden(part, low, mask):
        z1 = part + low.astype(f32)
        out = (jnp.maximum(z1 + bias_blocks, 0.0) * mask.astype(f32).T[:, :, None]).astype(bf16)
        out = lax.optimization_barrier(out)
        return [out, over_core(out)]

    sums_other = x_sums(keep_other, got_other)
    sums_own = x_sums(keep_own, got_own)
    hidden_other = hidden(*sums_other, mask_other)
    starts = [core * quarter, (1 - core) * quarter]
    cuts = [share // 2] * 4 + [share] * 2
    *for_other, w2 = fold(hidden_other, w2, cols2, scalars2, starts, [(n, bf16) for n in cuts], load=True, keep=True)
    got = []
    for part in for_other:
        got.append(over_depth(part))
    part_own, low_own, w2 = lax.optimization_barrier((*sums_own, w2))
    hidden_own = hidden(part_own, low_own, mask_own)
    mine = fold(hidden_own, w2, cols2, scalars2, starts, [(n, f32) for n in cuts])

    def over_col(parts, perm):
        return lax.ppermute(add(parts), "col", perm)

    cross = []
    for i in range(4):
        total = [mine[i], got[i]]
        total.append(over_col(total, [(0, 1), (3, 2)]))
        cross.append(over_col(total, [(1, 3), (2, 0)] if i < 2 else [(1, 2), (2, 1)]))
    near = over_col([mine[4], got[4]], [(i, i ^ 1) for i in range(size_col)])
    parts = [mine[5], got[5], near, *cross]
    return pl.pallas_call(
        finish_kernel,
        out_shape=jax.ShapeDtypeStruct((rows, share * block), bf16),
        compiler_params=pltpu.CompilerParams(vmem_limit_bytes=VMEM_LIMIT),
    )(*map(in_vmem, parts), bias2.reshape(share, block))


def fold_function(inputs, targets, stride):

    def add_tiles(running_total, tiles):

        def advance(number, total):
            offset = number * stride
            block_list = lax.dynamic_slice_in_dim(tiles, offset, stride, 0)
            incoming_rows = lax.dynamic_slice_in_dim(inputs, offset, stride, 1)
            wanted = lax.dynamic_slice_in_dim(targets, offset, stride, 0)
            product = jnp.einsum(
                "tws,wish->twih", incoming_rows, block_list, preferred_element_type=jnp.float32
            )
            flat_product = product.reshape(product.shape[0], -1, product.shape[-1])
            return total.at[:, wanted.reshape(-1)].add(flat_product)

        return lax.fori_loop(0, tiles.shape[0] // stride, advance, running_total)

    return add_tiles


def gather_plan(acts, act_mask, w1, cols1, bias1, mask2, w2, cols2, bias2):
    block = w1.shape[-1]
    rows_dev = acts.shape[0]
    row_blocks = act_mask.shape[1]
    col_blocks = mask2.shape[1]
    row_index = lax.axis_index("row")
    col_index = lax.axis_index("col")
    masked = acts.reshape(rows_dev, row_blocks, block) * act_mask[:, :, None].astype(jnp.bfloat16)
    first_targets = cols1 - col_index * col_blocks
    second_targets = cols2 - row_index * row_blocks
    first_fold = fold_function(masked, first_targets, w1.shape[0])
    first_sum = first_fold(
        jnp.zeros((rows_dev, col_blocks, block), jnp.float32), lax.all_gather(w1, "depth", axis=0, tiled=True)
    )
    bias_blocks = bias1.reshape(col_blocks, block)
    share = col_blocks // lax.axis_size("row")
    part_sum = lax.psum_scatter(first_sum, "row", scatter_dimension=1, tiled=True)
    bias_part = lax.dynamic_slice_in_dim(bias_blocks, row_index * share, share, 0)
    mask_part = lax.dynamic_slice_in_dim(mask2, row_index * share, share, 1)
    hidden_part = jnp.maximum(part_sum + bias_part, 0.0) * mask_part[:, :, None].astype(jnp.float32)
    hidden = lax.all_gather(hidden_part.astype(jnp.bfloat16), "row", axis=1, tiled=True)
    second_fold = fold_function(hidden, second_targets, w2.shape[0])
    second_sum = second_fold(
        jnp.zeros((rows_dev, row_blocks, block), jnp.float32), lax.all_gather(w2, "depth", axis=0, tiled=True)
    )
    outcome = lax.psum_scatter(second_sum, "col", scatter_dimension=1, tiled=True)
    bias_out = bias2.reshape(outcome.shape[1], block)
    return jnp.maximum(outcome + bias_out, 0.0).astype(jnp.bfloat16).reshape(rows_dev, -1)


def solution(mesh):
    sizes = dict(mesh.shape)
    pairs = sizes["depth"] == 2 and sizes["row"] == 4 and sizes["col"] == 4
    return jax.shard_map(
        exchange_plan if pairs else gather_plan,
        mesh=mesh,
        in_specs=(
            P("depth", "row"),
            P("depth", "row"),
            P(("row", "depth"), "col", None, None),
            P("row", "col"),
            P("col"),
            P("depth", "col"),
            P(("col", "depth"), "row", None, None),
            P("col", "row"),
            P(("row", "col")),
        ),
        out_specs=P("depth", ("row", "col")),
        check_vma=False,
    )
```
